32 devices in a mesh: blk: 8 (over z, y), band: 4 (over x, core).
Axes of the slice: x: 2, y: 2, z: 4, core: 2. Of those that a mesh axis runs over, the one named last changes fastest.
Arguments:
- grid_nodes: bfloat16 [16384, 512], P(('blk', 'band')), may hold values from -6 to 6
- enc_edges: bfloat16 [32768, 512], P(('blk', 'band')), may hold values from -6 to 6
- enc_sender: int32 [32768], P(('blk', 'band')), may hold values from 0 to 511, as said below
- enc_slot: int32 [32768], P(('blk', 'band')), may hold values from 0 to 511
- enc_slot_node: int32 [32, 512], P(('blk', 'band')), may hold values from 0 to 639
- mesh_nodes: bfloat16 [5120, 512], P('blk'), may hold values from -6 to 6
- mesh_edges: bfloat16 [32768, 512], P(('blk', 'band')), may hold values from -6 to 6
- mesh_sender: int32 [32768], P(('blk', 'band')), may hold values from 0 to 63
- mesh_receiver: int32 [32768], P(('blk', 'band')), may hold values from 0 to 639
- mesh_send_node: int32 [32, 64], P(('blk', 'band')), may hold values from 0 to 639
- grid_weights: bfloat16 [2, 512, 512], replicated, may hold values from -0.25 to 0.25
- enc_edge_weights: bfloat16 [4, 512, 512], replicated, may hold values from -0.25 to 0.25
- enc_node_weights: bfloat16 [3, 512, 512], replicated, may hold values from -0.25 to 0.25
- proc_edge_weights: bfloat16 [4, 512, 512], replicated, may hold values from -0.25 to 0.25
- proc_node_weights: bfloat16 [3, 512, 512], replicated, may hold values from -0.25 to 0.25
- biases: float32 [5, 2, 512], replicated, may hold values from -3 to 3
- gains: float32 [5, 512], replicated, may hold values from 0.5 to 1.5
Outputs:
- grid_out: bfloat16 [16384, 512], P(('blk', 'band'))
- mesh_out: bfloat16 [5120, 512], P(('blk', 'band'))
The draws below stay inside these ranges and needn't reach their ends.
Inputs may be any that keep to these rules, and one draw needn't show every extreme that they name: `enc_sender`: within each device's 1024 edges the values never fall, and every one of the device's 512 grid rows is a sender.
All inputs are finite; a program needn't handle non-finite values.
Results may differ from the reference program's by a relative error of at most 0.014.
Values may be sent and summed in bfloat16 or wider, within the bound.
No kernel may reach another device: no remote copies, remote signals or barrier semaphores. Data moves between devices by JAX's collectives and lax.ppermute only.
A program may use at most 64 MiB of HBM per device.

```python
import jax
import jax.numpy as jnp
from jax import lax

D = 512
GRID_DEV = 512
MESH_P = 640
MEDGE_DEV = 1024
NEIGH = 8
CAP = 64
MCAP = 8
EDGE_DEV = 1024
GRID = 16384
EDGES = 32768
MESH = 5120
MEDGES = 32768
N_BLK = 8
N_BAND = 4


def draw_enc_sender(key, part):
    devices = EDGES // EDGE_DEV
    extra_rows = jax.random.randint(key, (devices, EDGE_DEV - GRID_DEV), 0, GRID_DEV, dtype=jnp.int32)
    each_node = jnp.broadcast_to(jnp.arange(GRID_DEV, dtype=jnp.int32), (devices, GRID_DEV))
    return jnp.sort(jnp.concatenate([each_node, extra_rows], axis=1), axis=1).reshape(EDGES)


def draw_mesh_sender(key, part):
    key_near, key_offset, key_far, key_slot = jax.random.split(jax.random.fold_in(key, 17), 4)
    blk_index = jnp.arange(MEDGES, dtype=jnp.int32) // MEDGE_DEV // N_BAND
    nearby = jax.random.randint(key_near, (MEDGES,), 0, 4, dtype=jnp.int32) < 3
    offset = jax.random.randint(key_offset, (MEDGES,), 0, NEIGH, dtype=jnp.int32) - NEIGH // 2
    distant = jax.random.randint(key_far, (MEDGES,), 0, N_BLK, dtype=jnp.int32)
    patch = jnp.where(nearby, (blk_index + offset) % N_BLK, distant)
    slot = jax.random.randint(key_slot, (MEDGES,), 0, MCAP, dtype=jnp.int32)
    return (patch * MCAP + slot).astype(jnp.int32)


def place_ends(array, own_key, low, high):
    dims = array.shape
    spot = [jax.random.randint(jax.random.fold_in(own_key, axis), (), 0, dims[axis]) for axis in range(len(dims))]
    array = array.at[tuple(spot)].set(low)
    longest = dims.index(max(dims))
    spot[longest] = (spot[longest] + 1) % dims[longest]
    return array.at[tuple(spot)].set(high)


def block_scale(own_key, shape, cuts, least, largest):
    loudness, own = 1.0, jax.random.fold_in(own_key, 6)
    for dim, shards_of in cuts:
        heights = jnp.exp(jax.random.uniform(jax.random.fold_in(own, dim), (shards_of,), jnp.float32, least / len(cuts), largest / len(cuts)))
        loudness = loudness * jnp.repeat(heights, shape[dim] // shards_of).reshape([-1 if axis == dim else 1 for axis in range(len(shape))])
    return loudness


def scatter_about(rng, extent, scale, bound, shards=(), kind=jnp.bfloat16):
    result = scale * jax.random.normal(rng, extent, jnp.float32)
    if shards:
        result = result * block_scale(rng, extent, shards, -0.22, 0.18)
    return jnp.clip(result, -bound, bound).astype(kind)


def setup_inputs(seed: int = 0) -> dict:
    arg_keys = jax.random.split(jax.random.key(seed), 18)
    grid_nodes = scatter_about(arg_keys[0], (GRID, D), 1.0, 6.0, ((0, 32),))
    enc_edges = scatter_about(arg_keys[1], (EDGES, D), 1.0, 6.0, ((0, 32),))
    enc_sender = draw_enc_sender(jax.random.fold_in(arg_keys[17], 71), 0)
    enc_slot = place_ends(jax.random.randint(arg_keys[3], (EDGES,), 0, NEIGH * CAP), jax.random.fold_in(arg_keys[3], 1), 0, (NEIGH * CAP) - 1).astype(jnp.int32)
    enc_slot_node = place_ends(jax.random.randint(arg_keys[4], (N_BLK * N_BAND, NEIGH * CAP), 0, MESH_P), jax.random.fold_in(arg_keys[4], 1), 0, MESH_P - 1).astype(jnp.int32)
    mesh_nodes = scatter_about(arg_keys[5], (MESH, D), 1.0, 6.0, ((0, 8),))
    mesh_edges = scatter_about(arg_keys[6], (MEDGES, D), 1.0, 6.0, ((0, 32),))
    mesh_sender = draw_mesh_sender(jax.random.fold_in(arg_keys[17], 71), 0)
    mesh_receiver = place_ends(jax.random.randint(arg_keys[8], (MEDGES,), 0, MESH_P), jax.random.fold_in(arg_keys[8], 1), 0, MESH_P - 1).astype(jnp.int32)
    mesh_send_node = place_ends(jax.random.randint(arg_keys[9], (N_BLK * N_BAND, N_BLK * MCAP), 0, MESH_P), jax.random.fold_in(arg_keys[9], 1), 0, MESH_P - 1).astype(jnp.int32)
    grid_weights = scatter_about(arg_keys[10], (2, D, D), D ** -0.5, 0.25)
    enc_edge_weights = scatter_about(arg_keys[11], (4, D, D), D ** -0.5, 0.25)
    enc_node_weights = scatter_about(arg_keys[12], (3, D, D), D ** -0.5, 0.25)
    proc_edge_weights = scatter_about(arg_keys[13], (4, D, D), D ** -0.5, 0.25)
    proc_node_weights = scatter_about(arg_keys[14], (3, D, D), D ** -0.5, 0.25)
    biases = scatter_about(arg_keys[15], (5, 2, D), 0.5, 3.0, (), jnp.float32)
    gains = jnp.clip(1.0 + 0.1 * jax.random.normal(arg_keys[16], (5, D), jnp.float32), 0.5, 1.5)
    return {"grid_nodes": grid_nodes, "enc_edges": enc_edges, "enc_sender": enc_sender, "enc_slot": enc_slot, "enc_slot_node": enc_slot_node, "mesh_nodes": mesh_nodes, "mesh_edges": mesh_edges, "mesh_sender": mesh_sender, "mesh_receiver": mesh_receiver, "mesh_send_node": mesh_send_node, "grid_weights": grid_weights, "enc_edge_weights": enc_edge_weights, "enc_node_weights": enc_node_weights, "proc_edge_weights": proc_edge_weights, "proc_node_weights": proc_node_weights, "biases": biases, "gains": gains}


def layer_norm(values, gain_row):
    center = values - lax.optimization_barrier(jnp.mean(values, axis=-1, keepdims=True))
    spread = lax.optimization_barrier(jnp.mean(center * center, axis=-1, keepdims=True))
    return center * lax.rsqrt(spread + 1e-05) * gain_row

def dense_tail(first_layer, second_weight, bias_pair, gain_row):
    hidden = jax.nn.silu(first_layer + bias_pair[0]).astype(jnp.bfloat16)
    second = jnp.dot(hidden, second_weight, preferred_element_type=jnp.float32) + bias_pair[1]
    return layer_norm(second, gain_row)

def project(node_rows, weight):
    return jnp.dot(node_rows, weight, preferred_element_type=jnp.float32)

def reference(grid_nodes, enc_edges, enc_sender, enc_slot, enc_slot_node, mesh_nodes, mesh_edges, mesh_sender, mesh_receiver, mesh_send_node, grid_weights, enc_edge_weights, enc_node_weights, proc_edge_weights, proc_node_weights, biases, gains):
    grid_first = project(grid_nodes, grid_weights[0])
    grid_out = (grid_nodes.astype(jnp.float32) + dense_tail(grid_first, grid_weights[1], biases[0], gains[0])).astype(jnp.bfloat16)
    edge_device = jnp.arange(EDGES, dtype=jnp.int32) // EDGE_DEV
    edge_patch = edge_device // N_BAND
    edge_band = edge_device % N_BAND
    target_patch = (edge_patch + enc_slot // CAP - NEIGH // 2) % N_BLK
    slot_flat = enc_slot_node.reshape(-1)
    slot_index = (target_patch * N_BAND + edge_band) * (NEIGH * CAP) + enc_slot
    target_node = target_patch * MESH_P + slot_flat[slot_index]
    source_node = edge_device * GRID_DEV + enc_sender
    receiver_keys = project(mesh_nodes, enc_edge_weights[2]).astype(jnp.bfloat16)
    sender_proj = project(grid_nodes, enc_edge_weights[1])
    edge_first = project(enc_edges, enc_edge_weights[0]) + sender_proj[source_node] + receiver_keys[target_node].astype(jnp.float32)
    enc_message = dense_tail(edge_first, enc_edge_weights[3], biases[1], gains[1]).astype(jnp.bfloat16)
    enc_sum = jax.ops.segment_sum(enc_message.astype(jnp.float32), target_node, num_segments=MESH)
    node_first = project(mesh_nodes, enc_node_weights[0]) + project(enc_sum.astype(jnp.bfloat16), enc_node_weights[1])
    mesh_mid = (mesh_nodes.astype(jnp.float32) + dense_tail(node_first, enc_node_weights[2], biases[2], gains[2])).astype(jnp.bfloat16)
    mesh_device = jnp.arange(MEDGES, dtype=jnp.int32) // MEDGE_DEV
    mesh_patch = mesh_device // N_BAND
    mesh_band = mesh_device % N_BAND
    source_patch = mesh_sender // MCAP
    send_flat = mesh_send_node.reshape(-1)
    send_index = (source_patch * N_BAND + mesh_band) * (N_BLK * MCAP) + mesh_patch * MCAP + mesh_sender % MCAP
    mesh_source = source_patch * MESH_P + send_flat[send_index]
    mesh_target = mesh_patch * MESH_P + mesh_receiver
    sender_keys = project(mesh_mid, proc_edge_weights[1]).astype(jnp.bfloat16)
    target_keys = project(mesh_mid, proc_edge_weights[2]).astype(jnp.bfloat16)
    mesh_first = project(mesh_edges, proc_edge_weights[0]) + sender_keys[mesh_source].astype(jnp.float32) + target_keys[mesh_target].astype(jnp.float32)
    proc_message = dense_tail(mesh_first, proc_edge_weights[3], biases[3], gains[3]).astype(jnp.bfloat16)
    proc_sum = jax.ops.segment_sum(proc_message.astype(jnp.float32), mesh_target, num_segments=MESH)
    final_first = project(mesh_mid, proc_node_weights[0]) + project(proc_sum.astype(jnp.bfloat16), proc_node_weights[1])
    mesh_out = (mesh_mid.astype(jnp.float32) + dense_tail(final_first, proc_node_weights[2], biases[4], gains[4])).astype(jnp.bfloat16)
    return (grid_out, mesh_out)
```

```python
import jax
import jax.numpy as jnp
from jax import lax
from jax.sharding import PartitionSpec as P


NEIGH = 8
BF16 = jnp.bfloat16
F32 = jnp.float32


def layer_norm(values, gain_row):
    center = values - jnp.mean(values, axis=-1, keepdims=True)
    spread = jnp.mean(center * center, axis=-1, keepdims=True)
    return center * lax.rsqrt(spread + 1e-05) * gain_row


def dense_tail(first_layer, second_weight, bias_pair, gain_row):
    hidden = jax.nn.silu(first_layer + bias_pair[0]).astype(BF16)
    second = project(hidden, second_weight) + bias_pair[1]
    return layer_norm(second, gain_row)


def project(node_rows, weight):
    return jnp.dot(node_rows, weight, preferred_element_type=F32)


def pick_rows(indices, table):
    hot = (indices[:, None] == lax.broadcasted_iota(jnp.int32, (1, table.shape[0]), 1)).astype(BF16)
    return project(hot, table)


def sum_rows(indices, row_count, rows):
    hot = (lax.broadcasted_iota(jnp.int32, (row_count, 1), 0) == indices[None, :]).astype(BF16)
    return project(hot, rows)


def swap(rows, axis, mask):
    return lax.ppermute(rows, axis, [(i, i ^ mask) for i in range(lax.axis_size(axis))])


def window_exchange(blocks, back):
    blk_count = lax.axis_size("blk")
    pieces = []
    for window in range(NEIGH):
        if blk_count == NEIGH:
            pieces.append(swap(blocks[window], "blk", window) if window else blocks[0])
        else:
            distance = window - NEIGH // 2
            distance = distance if back else -distance
            route = [((i - distance) % blk_count, i) for i in range(blk_count)]
            pieces.append(lax.ppermute(blocks[window], "blk", route) if distance else blocks[window])
    return jnp.concatenate(pieces, axis=0)


def body(
    grid_nodes,
    enc_edges,
    enc_sender,
    enc_slot,
    enc_slot_node,
    mesh_nodes,
    mesh_edges,
    mesh_sender,
    mesh_receiver,
    mesh_send_node,
    grid_weights,
    enc_edge_weights,
    enc_node_weights,
    proc_edge_weights,
    proc_node_weights,
    biases,
    gains,
):
    blk_count, band_count = lax.axis_size("blk"), lax.axis_size("band")
    blk_index, band_index = lax.axis_index("blk"), lax.axis_index("band")
    patch_rows, width = mesh_nodes.shape
    share_rows = patch_rows // band_count
    slots = enc_slot_node.shape[1]
    cap = slots // NEIGH
    mcap = mesh_send_node.shape[1] // blk_count

    slot_nodes = enc_slot_node.reshape(NEIGH, cap)
    slot_place = enc_slot
    if blk_count == NEIGH:
        masks = jnp.arange(NEIGH)
        slot_nodes = jnp.take(slot_nodes, (blk_index - (blk_index ^ masks) + NEIGH // 2) % NEIGH, axis=0)
        patch = (blk_index + enc_slot // cap - NEIGH // 2) % NEIGH
        slot_place = (patch ^ blk_index) * cap + enc_slot % cap
    slot_nodes = slot_nodes.reshape(slots)

    slot_rows = pick_rows(slot_nodes, mesh_nodes).astype(BF16)
    slot_keys = project(slot_rows, enc_edge_weights[2]).astype(BF16).reshape(NEIGH, cap, width)
    arrived_keys = window_exchange(slot_keys, False)

    sender_rows = pick_rows(enc_sender, grid_nodes).astype(BF16)
    edge_part = project(enc_edges, enc_edge_weights[0]) + project(sender_rows, enc_edge_weights[1])
    grid_out = (
        grid_nodes.astype(F32)
        + dense_tail(project(grid_nodes, grid_weights[0]), grid_weights[1], biases[0], gains[0])
    ).astype(BF16)

    edge_first = edge_part + pick_rows(slot_place, arrived_keys)
    enc_message = dense_tail(edge_first, enc_edge_weights[3], biases[1], gains[1]).astype(BF16)
    slot_sums = sum_rows(slot_place, slots, enc_message).astype(BF16).reshape(NEIGH, cap, width)
    landed = window_exchange(slot_sums, True)
    partial_sums = sum_rows(slot_nodes, patch_rows, landed)

    low = band_index % 2
    quarters = partial_sums.reshape(band_count // 2, 2, share_rows, width)
    kept = lax.dynamic_index_in_dim(quarters, low, 1, False)
    given = lax.dynamic_index_in_dim(quarters, 1 - low, 1, False).astype(BF16)
    half = (kept + swap(given, "band", 1).astype(F32)).astype(BF16)
    mask = 2
    while mask < band_count:
        half = (half.astype(F32) + swap(half, "band", mask).astype(F32)).astype(BF16)
        mask *= 2
    half_rows = patch_rows // 2
    enc_total = half.reshape(half_rows, width)
    own_nodes = lax.dynamic_index_in_dim(
        mesh_nodes.reshape(band_count // 2, 2, share_rows, width), low, 1, False
    ).reshape(half_rows, width)
    node_first = project(own_nodes, enc_node_weights[0]) + project(enc_total, enc_node_weights[1])
    half_mid = (
        own_nodes.astype(F32) + dense_tail(node_first, enc_node_weights[2], biases[2], gains[2])
    ).astype(BF16)
    other_mid = swap(half_mid, "band", 1)
    all_mid = jnp.concatenate([half_mid, other_mid], axis=0)

    def mid_place(node):
        share = node // share_rows
        return ((share % 2) ^ low) * half_rows + (share // 2) * share_rows + node % share_rows

    send_nodes = jnp.take(mesh_send_node.reshape(blk_count, mcap), blk_index ^ jnp.arange(blk_count), axis=0)
    wanted = pick_rows(mid_place(send_nodes.reshape(-1)), all_mid).astype(BF16)
    senders = project(wanted, proc_edge_weights[1]).astype(BF16).reshape(blk_count, mcap, width)
    mask = 1
    while mask < blk_count:
        view = senders.reshape(blk_count // (2 * mask), 2, mask * mcap, width)
        got = swap(view[:, 1], "blk", mask)
        senders = jnp.stack([view[:, 0], got], axis=1)
        mask *= 2
    arrived_senders = senders.reshape(blk_count * mcap, width)
    sender_place = ((mesh_sender // mcap) ^ blk_index) * mcap + mesh_sender % mcap

    target_keys = project(all_mid, proc_edge_weights[2]).astype(BF16)
    mesh_first = (
        project(mesh_edges, proc_edge_weights[0])
        + pick_rows(sender_place, arrived_senders)
        + pick_rows(mid_place(mesh_receiver), target_keys)
    )
    proc_message = dense_tail(mesh_first, proc_edge_weights[3], biases[3], gains[3]).astype(BF16)
    shares = sum_rows(mesh_receiver, patch_rows, proc_message)
    shares = shares.reshape(band_count, share_rows, width)
    place, mask = band_index, 1
    while mask < band_count:
        pairs = shares.reshape(-1, 2, share_rows, width)
        kept = lax.dynamic_index_in_dim(pairs, place % 2, 1, False)
        given = lax.dynamic_index_in_dim(pairs, 1 - place % 2, 1, False).astype(BF16)
        shares = kept + swap(given, "band", mask).astype(F32)
        place, mask = place // 2, mask * 2
    proc_total = shares.reshape(share_rows, width).astype(BF16)
    own_mid = lax.dynamic_index_in_dim(
        half_mid.reshape(band_count // 2, share_rows, width), band_index // 2, 0, False
    )
    final_first = project(own_mid, proc_node_weights[0]) + project(proc_total, proc_node_weights[1])
    mesh_out = (
        own_mid.astype(F32) + dense_tail(final_first, proc_node_weights[2], biases[4], gains[4])
    ).astype(BF16)
    return (grid_out, mesh_out)


def solution(mesh):
    rows = P(("blk", "band"), None)
    flat = P(("blk", "band"))
    in_specs = (rows, rows, flat, flat, rows, P("blk", None), rows, flat, flat, rows) + (P(),) * 7
    return jax.shard_map(
        body, mesh=mesh, in_specs=in_specs, out_specs=(rows, rows), check_vma=False
    )
```

```python
import functools

import jax
import jax.numpy as jnp
from jax import lax
from jax.experimental import pallas as pl
from jax.experimental.pallas import tpu as pltpu
from jax.sharding import PartitionSpec as P


NEIGH = 8
BF16 = jnp.bfloat16
F32 = jnp.float32
TILE = 256


def project(node_rows, weight):
    return jnp.dot(node_rows, weight, preferred_element_type=F32)


def silu(values):
    half = values * 0.5
    return half + half * jnp.tanh(half)


def normed(second, gain_row):
    center = second - jnp.mean(second, axis=-1, keepdims=True)
    spread = jnp.mean(center * center, axis=-1, keepdims=True)
    return center * (lax.rsqrt(spread + 1e-05) * gain_row)


def tail(first, weight_ref, biases_ref, gains_ref, block):
    hidden = silu(first).astype(BF16)
    second = project(hidden, weight_ref[...]) + biases_ref[block, 1:2, :]
    return normed(second, gains_ref[block : block + 1, :])


def column(row):
    return jnp.broadcast_to(row, (128, row.shape[1])).T


def hot_columns(indices, names):
    wide = names.shape[1]
    if wide <= 128:
        return (indices[:, :wide] == names).astype(F32).astype(BF16)
    parts = [
        (indices == names[:, at : at + 128]).astype(F32).astype(BF16) for at in range(0, wide, 128)
    ]
    return jnp.concatenate(parts, axis=1)


def hot_rows(row, names):
    return (row == names).astype(F32).astype(BF16)


def lanes(count):
    return lax.broadcasted_iota(jnp.int32, (1, count), 1)


def sublanes(count):
    return lax.broadcasted_iota(jnp.int32, (count, 1), 0)


def share_names(iota, share_rows, band_count, core):
    half_count = band_count // 2
    names = iota
    for place in range(band_count):
        share = 2 * (place % half_count) + (core if place < half_count else 1 - core)
        offset = (share - place) * share_rows
        inside = (iota >= place * share_rows) & (iota < (place + 1) * share_rows)
        names = jnp.where(inside, iota + offset, names)
    return names


def call(kernel, outs, args, scratch=(), flops=0):
    single = not isinstance(outs, (list, tuple))
    return pl.pallas_call(
        kernel,
        out_shape=outs if single else tuple(outs),
        in_specs=[pl.BlockSpec(memory_space=pltpu.VMEM)] * len(args),
        out_specs=pl.BlockSpec(memory_space=pltpu.VMEM)
        if single
        else (pl.BlockSpec(memory_space=pltpu.VMEM),) * len(outs),
        scratch_shapes=list(scratch),
        cost_estimate=pl.CostEstimate(flops=flops, transcendentals=0, bytes_accessed=0),
    )(*args)


def shape(dims, kind):
    return jax.ShapeDtypeStruct(dims, kind)


def window_of(mask, exact, blk_count):
    if not exact:
        return mask
    blk = lax.axis_index("blk")
    return (blk - (blk ^ mask) + NEIGH // 2 + blk_count) % NEIGH


def keys_kernel(exact, blk_count, node_ref, mesh_ref, weight_ref, *refs):
    outs, held = refs[:NEIGH], refs[NEIGH]
    picks = hot_columns(column(node_ref[...]), lanes(mesh_ref.shape[0]))
    rows = project(picks, mesh_ref[...]).astype(BF16)
    keys = project(rows, weight_ref[...]).astype(BF16)
    held[...] = keys.reshape(held.shape)
    for mask in range(NEIGH):
        outs[mask][...] = held[window_of(mask, exact, blk_count)]


def local_kernel(
    sender_ref, grid_ref, edges_ref, w_edge, w_sender, w_grid, w_grid_last, biases_ref, gains_ref, part_ref, out_ref
):
    rows = grid_ref.shape[0]
    names = lanes(rows)
    senders = column(sender_ref[...])
    for at in range(0, edges_ref.shape[0], TILE):
        picks = hot_columns(senders[at : at + TILE], names)
        nodes = project(picks, grid_ref[...]).astype(BF16)
        part_ref[at : at + TILE, :] = (
            project(edges_ref[at : at + TILE, :], w_edge[...])
            + project(nodes, w_sender[...])
            + biases_ref[1, 0:1, :]
        )
    for at in range(0, rows, TILE):
        nodes = grid_ref[at : at + TILE, :]
        first = project(nodes, w_grid[...]) + biases_ref[0, 0:1, :]
        out_ref[at : at + TILE, :] = (
            nodes.astype(F32) + tail(first, w_grid_last, biases_ref, gains_ref, 0)
        ).astype(BF16)


def message_kernel(slot_ref, part_ref, weight_ref, biases_ref, gains_ref, *refs):
    keys, outs, table, sent = refs[:NEIGH], refs[NEIGH : 2 * NEIGH], refs[-2], refs[-1]
    cap = keys[0].shape[0]
    for window in range(NEIGH):
        table[window * cap : (window + 1) * cap, :] = keys[window][...]
    slots = column(slot_ref[...])
    names = lanes(table.shape[0])
    for at in range(0, part_ref.shape[0], TILE):
        picks = hot_columns(slots[at : at + TILE], names)
        first = part_ref[at : at + TILE, :] + project(picks, table[...])
        sent[at : at + TILE, :] = tail(first, weight_ref, biases_ref, gains_ref, 1).astype(BF16)
    sums = project(hot_rows(slot_ref[...], sublanes(table.shape[0])), sent[...]).astype(BF16)
    for window in range(NEIGH):
        outs[window][...] = sums[window * cap : (window + 1) * cap, :]


def land_kernel(exact, blk_count, band_count, node_ref, *refs):
    pieces, given_ref, kept_ref, held = refs[:NEIGH], refs[NEIGH], refs[NEIGH + 1], refs[NEIGH + 2]
    for mask in range(NEIGH):
        held[window_of(mask, exact, blk_count)] = pieces[mask][...]
    half = given_ref.shape[0]
    core = lax.axis_index("band") % 2
    names = share_names(sublanes(2 * half), 2 * half // band_count, band_count, 1 - core)
    landed = held[...].reshape(-1, held.shape[2])
    given_ref[...] = project(hot_rows(node_ref[...], names[:half]), landed).astype(BF16)
    kept_ref[...] = project(hot_rows(node_ref[...], names[half:]), landed)


def early_kernel(band_count, nodes_ref, edges_ref, w_node, w_edge, biases_ref, node_part_ref, edge_part_ref):
    core = lax.axis_index("band") % 2
    share = node_part_ref.shape[0] // (band_count // 2)
    for place in range(band_count // 2):
        rows = nodes_ref[2 * place + core]
        node_part_ref[place * share : (place + 1) * share, :] = (
            project(rows, w_node[...]) + biases_ref[2, 0:1, :]
        )
    for at in range(0, edges_ref.shape[0], TILE):
        edge_part_ref[at : at + TILE, :] = (
            project(edges_ref[at : at + TILE, :], w_edge[...]) + biases_ref[3, 0:1, :]
        )


def node_kernel(band_count, halves, *refs):
    sums, rest = refs[:halves], refs[halves:]
    nodes_ref, part_ref, w_sum, w_last, biases_ref, gains_ref, out_ref = rest
    core = lax.axis_index("band") % 2
    share = out_ref.shape[0] // (band_count // 2)
    total = sums[0][...].astype(F32)
    for other in sums[1:]:
        total = total + other[...].astype(F32)
    first = part_ref[...] + project(total.astype(BF16), w_sum[...])
    change = tail(first, w_last, biases_ref, gains_ref, 2)
    for place in range(band_count // 2):
        at = place * share
        out_ref[at : at + share, :] = (
            nodes_ref[2 * place + core].astype(F32) + change[at : at + share, :]
        ).astype(BF16)


def sender_kernel(band_count, send_ref, own_ref, other_ref, weight_ref, out_ref, table):
    half = own_ref.shape[0]
    table[:half, :] = own_ref[...]
    table[half:, :] = other_ref[...]
    core = lax.axis_index("band") % 2
    names = share_names(lanes(2 * half), 2 * half // band_count, band_count, core)
    rows = project(hot_columns(column(send_ref[...]), names), table[...]).astype(BF16)
    out_ref[...] = project(rows, weight_ref[...]).astype(BF16)


def target_kernel(band_count, receiver_ref, own_ref, other_ref, part_ref, weight_ref, out_ref, table):
    half = own_ref.shape[0]
    table[:half, :] = project(own_ref[...], weight_ref[...]).astype(BF16)
    table[half:, :] = project(other_ref[...], weight_ref[...]).astype(BF16)
    core = lax.axis_index("band") % 2
    names = share_names(lanes(2 * half), 2 * half // band_count, band_count, core)
    receivers = column(receiver_ref[...])
    for at in range(0, part_ref.shape[0], TILE):
        picks = hot_columns(receivers[at : at + TILE], names)
        out_ref[at : at + TILE, :] = part_ref[at : at + TILE, :] + project(picks, table[...])


def process_kernel(
    band_count, sender_ref, receiver_ref, part_ref, keys_ref, weight_ref, biases_ref, gains_ref, given_ref, kept_ref, sent
):
    senders = column(sender_ref[...])
    names = lanes(keys_ref.shape[0])
    for at in range(0, part_ref.shape[0], TILE):
        picks = hot_columns(senders[at : at + TILE], names)
        first = part_ref[at : at + TILE, :] + project(picks, keys_ref[...])
        sent[at : at + TILE, :] = tail(first, weight_ref, biases_ref, gains_ref, 3).astype(BF16)
    half = given_ref.shape[0]
    core = lax.axis_index("band") % 2
    places = share_names(sublanes(2 * half), 2 * half // band_count, band_count, 1 - core)
    given_ref[...] = project(hot_rows(receiver_ref[...], places[:half]), sent[...]).astype(BF16)
    kept_ref[...] = project(hot_rows(receiver_ref[...], places[half:]), sent[...])


def last_kernel(kept_ref, got_ref, own_ref, w_node, w_sum, w_last, biases_ref, gains_ref, out_ref):
    total = (kept_ref[...] + got_ref[...].astype(F32)).astype(BF16)
    first = (
        project(own_ref[...], w_node[...]) + project(total, w_sum[...]) + biases_ref[4, 0:1, :]
    )
    out_ref[...] = (
        own_ref[...].astype(F32) + tail(first, w_last, biases_ref, gains_ref, 4)
    ).astype(BF16)


def swap(rows, axis, mask):
    return lax.ppermute(rows, axis, [(i, i ^ mask) for i in range(lax.axis_size(axis))])


def window_exchange(blocks, back):
    blk_count = lax.axis_size("blk")
    pieces = []
    for window in range(NEIGH):
        if blk_count == NEIGH:
            pieces.append(swap(blocks[window], "blk", window) if window else blocks[0])
        else:
            distance = window - NEIGH // 2
            distance = distance if back else -distance
            route = [((i - distance) % blk_count, i) for i in range(blk_count)]
            pieces.append(lax.ppermute(blocks[window], "blk", route) if distance else blocks[window])
    return pieces


def body(
    grid_nodes,
    enc_edges,
    enc_sender,
    enc_slot,
    enc_slot_node,
    mesh_nodes,
    mesh_edges,
    mesh_sender,
    mesh_receiver,
    mesh_send_node,
    grid_weights,
    enc_edge_weights,
    enc_node_weights,
    proc_edge_weights,
    proc_node_weights,
    biases,
    gains,
):
    blk_count, band_count = lax.axis_size("blk"), lax.axis_size("band")
    blk_index, band_index = lax.axis_index("blk"), lax.axis_index("band")
    patch_rows, width = mesh_nodes.shape
    share_rows, half_rows = patch_rows // band_count, patch_rows // 2
    edge_rows, grid_rows, medge_rows = enc_edges.shape[0], grid_nodes.shape[0], mesh_edges.shape[0]
    slots = enc_slot_node.shape[1]
    cap = slots // NEIGH
    senders_all = mesh_send_node.shape[1]
    mcap = senders_all // blk_count
    exact = blk_count == NEIGH
    unit = 2 * width * width
    bf_piece = shape((cap, width), BF16)

    slot_place = enc_slot
    if exact:
        patch = (blk_index + lax.div(enc_slot, cap) + NEIGH // 2) % NEIGH
        slot_place = (patch ^ blk_index) * cap + lax.rem(enc_slot, cap)
    slot_place = slot_place.reshape(1, edge_rows)

    slot_keys = call(
        functools.partial(keys_kernel, exact, blk_count),
        [bf_piece] * NEIGH,
        (enc_slot_node, mesh_nodes, enc_edge_weights[2]),
        [pltpu.VMEM((NEIGH, cap, width), BF16)],
        unit * 2 * slots,
    )
    keys = window_exchange(slot_keys, False)

    edge_part, grid_out = call(
        local_kernel,
        [shape((edge_rows, width), F32), shape((grid_rows, width), BF16)],
        (
            enc_sender.reshape(1, edge_rows),
            grid_nodes,
            enc_edges,
            enc_edge_weights[0],
            enc_edge_weights[1],
            grid_weights[0],
            grid_weights[1],
            biases,
            gains,
        ),
        (),
        unit * (3 * edge_rows + 2 * grid_rows),
    )

    slot_sums = call(
        message_kernel,
        [bf_piece] * NEIGH,
        (slot_place, edge_part, enc_edge_weights[3], biases, gains, *keys),
        [pltpu.VMEM((slots, width), BF16), pltpu.VMEM((edge_rows, width), BF16)],
        unit * 3 * edge_rows,
    )
    landed = window_exchange(slot_sums, True)

    nodes_by_share = mesh_nodes.reshape(band_count, share_rows, width)
    node_part, mesh_part = call(
        functools.partial(early_kernel, band_count),
        [shape((half_rows, width), F32), shape((medge_rows, width), F32)],
        (nodes_by_share, mesh_edges, enc_node_weights[0], proc_edge_weights[0], biases),
        (),
        unit * (half_rows + medge_rows),
    )

    half_bf, half_f = shape((half_rows, width), BF16), shape((half_rows, width), F32)
    given, kept = call(
        functools.partial(land_kernel, exact, blk_count, band_count),
        [half_bf, half_f],
        (enc_slot_node, *landed),
        [pltpu.VMEM((NEIGH, cap, width), BF16)],
        unit * patch_rows,
    )
    half = (kept + swap(given, "band", 1).astype(F32)).astype(BF16)
    mask, halves = 2, (half,)
    while mask < band_count:
        if len(halves) == 2:
            half = (halves[0].astype(F32) + halves[1].astype(F32)).astype(BF16)
        halves = (half, swap(half, "band", mask))
        mask *= 2
    half_mid = call(
        functools.partial(node_kernel, band_count, len(halves)),
        half_bf,
        (*halves, nodes_by_share, node_part, enc_node_weights[1], enc_node_weights[2], biases, gains),
        (),
        unit * 2 * half_rows,
    )
    other_mid = swap(half_mid, "band", 1)

    send_nodes = jnp.take(
        mesh_send_node.reshape(blk_count, mcap), blk_index ^ jnp.arange(blk_count), axis=0, mode="clip"
    ).reshape(1, senders_all)
    senders = call(
        functools.partial(sender_kernel, band_count),
        shape((senders_all, width), BF16),
        (send_nodes, half_mid, other_mid, proc_edge_weights[1]),
        [pltpu.VMEM((patch_rows, width), BF16)],
        unit * 2 * senders_all,
    ).reshape(blk_count, mcap, width)
    mask = 1
    while mask < blk_count:
        view = senders.reshape(blk_count // (2 * mask), 2, mask * mcap, width)
        got = swap(view[:, 1], "blk", mask)
        senders = jnp.stack([view[:, 0], got], axis=1)
        mask *= 2
    arrived_senders = senders.reshape(senders_all, width)
    sender_place = (
        (lax.div(mesh_sender, mcap) ^ blk_index) * mcap + lax.rem(mesh_sender, mcap)
    ).reshape(1, medge_rows)
    receivers = mesh_receiver.reshape(1, medge_rows)

    mesh_part = call(
        functools.partial(target_kernel, band_count),
        shape((medge_rows, width), F32),
        (receivers, half_mid, other_mid, mesh_part, proc_edge_weights[2]),
        [pltpu.VMEM((patch_rows, width), BF16)],
        unit * (patch_rows + medge_rows),
    )
    given, kept = call(
        functools.partial(process_kernel, band_count),
        [half_bf, half_f],
        (sender_place, receivers, mesh_part, arrived_senders, proc_edge_weights[3], biases, gains),
        [pltpu.VMEM((medge_rows, width), BF16)],
        unit * 3 * medge_rows,
    )
    shares = kept + swap(given, "band", 1).astype(F32)
    shares = shares.reshape(band_count // 2, share_rows, width)
    got = jnp.zeros((1, share_rows, width), BF16)
    place, mask = band_index // 2, 2
    while mask < band_count:
        pairs = shares.reshape(-1, 2, share_rows, width)
        kept = lax.dynamic_index_in_dim(pairs, place % 2, 1, False)
        given = lax.dynamic_index_in_dim(pairs, 1 - place % 2, 1, False).astype(BF16)
        got = swap(given, "band", mask)
        place, mask = place // 2, mask * 2
        if mask < band_count:
            shares = kept + got.astype(F32)
    own_mid = lax.dynamic_index_in_dim(
        half_mid.reshape(band_count // 2, share_rows, width), band_index // 2, 0, False
    )
    mesh_out = call(
        last_kernel,
        shape((share_rows, width), BF16),
        (
            kept.reshape(share_rows, width),
            got.reshape(share_rows, width),
            own_mid,
            proc_node_weights[0],
            proc_node_weights[1],
            proc_node_weights[2],
            biases,
            gains,
        ),
        (),
        unit * 3 * share_rows,
    )
    return (grid_out, mesh_out)


def solution(mesh):
    rows = P(("blk", "band"), None)
    flat = P(("blk", "band"))
    in_specs = (rows, rows, flat, flat, rows, P("blk", None), rows, flat, flat, rows) + (P(),) * 7
    return jax.shard_map(
        body, mesh=mesh, in_specs=in_specs, out_specs=(rows, rows), check_vma=False
    )
```

```python
import functools

import jax
import jax.numpy as jnp
from jax import lax
from jax.experimental import pallas as pl
from jax.experimental.pallas import tpu as pltpu
from jax.sharding import PartitionSpec as P


NEIGH = 8
BF16 = jnp.bfloat16
F32 = jnp.float32
TILE = 256
GRANT = 16 << 20


def project(node_rows, weight):
    return jnp.dot(node_rows, weight, preferred_element_type=F32)


def silu(values):
    half = values * 0.5
    return half + half * jnp.tanh(half)


def normed(second, gain_row):
    center = second - jnp.mean(second, axis=-1, keepdims=True)
    spread = jnp.mean(center * center, axis=-1, keepdims=True)
    return center * (lax.rsqrt(spread + 1e-05) * gain_row)


def tail(first, weight, biases_ref, gains_ref, block):
    hidden = silu(first).astype(BF16)
    second = project(hidden, weight) + biases_ref[block, 1:2, :]
    return normed(second, gains_ref[block : block + 1, :])


def column(row):
    return jnp.broadcast_to(row, (128, row.shape[1])).T


def hot_columns(indices, names):
    wide = names.shape[1]
    if wide <= 128:
        return (indices[:, :wide] == names).astype(F32).astype(BF16)
    parts = [
        (indices == names[:, at : at + 128]).astype(F32).astype(BF16) for at in range(0, wide, 128)
    ]
    return jnp.concatenate(parts, axis=1)


def hot_rows(row, names):
    return (row == names).astype(F32).astype(BF16)


def lanes(count):
    return lax.broadcasted_iota(jnp.int32, (1, count), 1)


def sublanes(count):
    return lax.broadcasted_iota(jnp.int32, (count, 1), 0)


def share_names(iota, share_rows, band_count, core):
    half_count = band_count // 2
    x = lax.div(lax.axis_index("band"), 2)
    names = iota
    for place in range(band_count):
        share = 2 * ((place % half_count) ^ x) + (core if place < half_count else 1 - core)
        offset = (share - place) * share_rows
        inside = (iota >= place * share_rows) & (iota < (place + 1) * share_rows)
        names = jnp.where(inside, iota + offset, names)
    return names


def call(kernel, outs, args, scratch=(), flops=0, in_hbm=()):
    single = not isinstance(outs, (list, tuple))
    outs = [outs] if single else outs
    vmem = pl.BlockSpec(memory_space=pltpu.VMEM)
    args = [
        arg if at in in_hbm else pltpu.with_memory_space_constraint(arg, pltpu.VMEM)
        for at, arg in enumerate(args)
    ]
    results = pl.pallas_call(
        kernel,
        out_shape=tuple(pltpu.VMEM(out.shape, out.dtype) for out in outs),
        in_specs=[
            pl.BlockSpec(memory_space=pl.ANY) if at in in_hbm else vmem for at in range(len(args))
        ],
        out_specs=(vmem,) * len(outs),
        scratch_shapes=list(scratch),
        cost_estimate=pl.CostEstimate(flops=flops, transcendentals=0, bytes_accessed=0),
        compiler_params=pltpu.CompilerParams(vmem_limit_bytes=GRANT),
    )(*args)
    return results[0] if single else results


def shape(dims, kind):
    return jax.ShapeDtypeStruct(dims, kind)


def window_of(mask, exact):
    if not exact:
        return mask
    blk = lax.axis_index("blk")
    return lax.rem(blk - (blk ^ mask) + NEIGH // 2 + NEIGH, NEIGH)


def keys_kernel(exact, node_ref, mesh_hbm, weights_hbm, *refs):
    outs, (held, mesh, weight, sems) = refs[:NEIGH], refs[NEIGH:]
    get_mesh = pltpu.make_async_copy(mesh_hbm, mesh, sems.at[0])
    get_weight = pltpu.make_async_copy(weights_hbm.at[2], weight, sems.at[1])
    get_mesh.start()
    get_weight.start()
    picks = hot_columns(column(node_ref[...]), lanes(mesh.shape[0]))
    get_mesh.wait()
    rows = project(picks, mesh[...]).astype(BF16)
    get_weight.wait()
    keys = project(rows, weight[...]).astype(BF16)
    held[...] = keys.reshape(held.shape)
    for mask in range(NEIGH):
        outs[mask][...] = held[window_of(mask, exact)]


def edge_kernel(sender_ref, grid_ref, edges_ref, weights_ref, biases_ref, part_ref):
    names = lanes(grid_ref.shape[0])
    senders = column(sender_ref[...])
    for at in range(0, edges_ref.shape[0], TILE):
        picks = hot_columns(senders[at : at + TILE], names)
        nodes = project(picks, grid_ref[...]).astype(BF16)
        part_ref[at : at + TILE, :] = (
            project(edges_ref[at : at + TILE, :], weights_ref[0])
            + project(nodes, weights_ref[1])
            + biases_ref[1, 0:1, :]
        )


def grid_kernel(grid_ref, weights_ref, biases_ref, gains_ref, out_ref):
    for at in range(0, grid_ref.shape[0], TILE):
        nodes = grid_ref[at : at + TILE, :]
        first = project(nodes, weights_ref[0]) + biases_ref[0, 0:1, :]
        out_ref[at : at + TILE, :] = (
            nodes.astype(F32) + tail(first, weights_ref[1], biases_ref, gains_ref, 0)
        ).astype(BF16)


def message_kernel(exact, slot_ref, part_ref, weights_ref, biases_ref, gains_ref, *refs):
    keys, outs, table, sent = refs[:NEIGH], refs[NEIGH : 2 * NEIGH], refs[-2], refs[-1]
    cap = keys[0].shape[0]
    for window in range(NEIGH):
        table[window * cap : (window + 1) * cap, :] = keys[window][...]
    row = slot_ref[...]
    if exact:
        blk = lax.axis_index("blk")
        patch = (lax.div(row, cap) + (blk + NEIGH // 2)) & (NEIGH - 1)
        row = (patch ^ blk) * cap + lax.rem(row, cap)
    slots = column(row)
    names = lanes(table.shape[0])
    for at in range(0, part_ref.shape[0], TILE):
        picks = hot_columns(slots[at : at + TILE], names)
        first = part_ref[at : at + TILE, :] + project(picks, table[...])
        sent[at : at + TILE, :] = tail(first, weights_ref[3], biases_ref, gains_ref, 1).astype(BF16)
    sums = project(hot_rows(row, sublanes(table.shape[0])), sent[...]).astype(BF16)
    for window in range(NEIGH):
        outs[window][...] = sums[window * cap : (window + 1) * cap, :]


def land_kernel(exact, band_count, node_ref, *refs):
    pieces, given_ref, kept_ref, held = refs[:NEIGH], refs[NEIGH], refs[NEIGH + 1], refs[NEIGH + 2]
    for mask in range(NEIGH):
        held[window_of(mask, exact)] = pieces[mask][...]
    half = given_ref.shape[0]
    core = lax.rem(lax.axis_index("band"), 2)
    names = share_names(sublanes(2 * half), 2 * half // band_count, band_count, 1 - core)
    landed = held[...].reshape(-1, held.shape[2])
    given_ref[...] = project(hot_rows(node_ref[...], names[:half]), landed).astype(BF16)
    kept_ref[...] = project(hot_rows(node_ref[...], names[half:]), landed)


def own_share(place):
    band = lax.axis_index("band")
    return 2 * (place ^ lax.div(band, 2)) + lax.rem(band, 2)


def early_kernel(band_count, nodes_ref, edges_ref, w_nodes, w_edges, biases_ref, node_part_ref, edge_part_ref):
    share = node_part_ref.shape[0] // (band_count // 2)
    for place in range(band_count // 2):
        node_part_ref[place * share : (place + 1) * share, :] = (
            project(nodes_ref[own_share(place)], w_nodes[0]) + biases_ref[2, 0:1, :]
        )
    for at in range(0, edges_ref.shape[0], TILE):
        edge_part_ref[at : at + TILE, :] = (
            project(edges_ref[at : at + TILE, :], w_edges[0]) + biases_ref[3, 0:1, :]
        )


def node_kernel(band_count, bit, half_ref, got_ref, nodes_ref, part_ref, weights_ref, biases_ref, gains_ref, out_ref):
    share = out_ref.shape[0] // (band_count // 2)
    total = crossed(half_ref, got_ref, share, band_count, bit)
    first = part_ref[...] + project(total, weights_ref[1])
    change = tail(first, weights_ref[2], biases_ref, gains_ref, 2)
    for place in range(band_count // 2):
        at = place * share
        out_ref[at : at + share, :] = (
            nodes_ref[own_share(place)].astype(F32) + change[at : at + share, :]
        ).astype(BF16)


def crossed(half, got, share, band_count, bit):
    parts = []
    for place in range(band_count // 2):
        at, other = place * share, (place ^ bit) * share
        parts.append(half[at : at + share, :].astype(F32) + got[other : other + share, :].astype(F32))
    return jnp.concatenate(parts, axis=0).astype(BF16)


def sender_kernel(band_count, send_ref, own_ref, other_ref, weights_ref, kept_ref, given_ref, table, held):
    half = own_ref.shape[0]
    table[:half, :] = own_ref[...]
    table[half:, :] = other_ref[...]
    core = lax.rem(lax.axis_index("band"), 2)
    names = share_names(lanes(2 * half), 2 * half // band_count, band_count, core)
    rows = project(hot_columns(column(send_ref[...]), names), table[...]).astype(BF16)
    held[...] = project(rows, weights_ref[1]).astype(BF16).reshape(held.shape)
    blk = lax.axis_index("blk")
    for pair in range(kept_ref.shape[0]):
        kept_ref[pair] = held[blk ^ (2 * pair)]
        given_ref[pair] = held[blk ^ (2 * pair + 1)]


def target_kernel(band_count, receiver_ref, own_ref, other_ref, part_ref, weights_ref, out_ref, table):
    half = own_ref.shape[0]
    table[:half, :] = project(own_ref[...], weights_ref[2]).astype(BF16)
    table[half:, :] = project(other_ref[...], weights_ref[2]).astype(BF16)
    core = lax.rem(lax.axis_index("band"), 2)
    names = share_names(lanes(2 * half), 2 * half // band_count, band_count, core)
    receivers = column(receiver_ref[...])
    for at in range(0, part_ref.shape[0], TILE):
        picks = hot_columns(receivers[at : at + TILE], names)
        out_ref[at : at + TILE, :] = part_ref[at : at + TILE, :] + project(picks, table[...])


def process_kernel(
    band_count, mcap, sender_ref, receiver_ref, part_ref, keys_ref, weights_ref, biases_ref, gains_ref, given_ref, kept_ref, sent
):
    senders = column(sender_ref[...] ^ (lax.axis_index("blk") * mcap))
    names = lanes(keys_ref.shape[0])
    for at in range(0, part_ref.shape[0], TILE):
        picks = hot_columns(senders[at : at + TILE], names)
        first = part_ref[at : at + TILE, :] + project(picks, keys_ref[...])
        sent[at : at + TILE, :] = tail(first, weights_ref[3], biases_ref, gains_ref, 3).astype(BF16)
    half = given_ref.shape[0]
    core = lax.rem(lax.axis_index("band"), 2)
    places = share_names(sublanes(2 * half), 2 * half // band_count, band_count, 1 - core)
    given_ref[...] = project(hot_rows(receiver_ref[...], places[:half]), sent[...]).astype(BF16)
    kept_ref[...] = project(hot_rows(receiver_ref[...], places[half:]), sent[...])


def last_kernel(kept_ref, got_ref, half_ref, weights_ref, biases_ref, gains_ref, out_ref):
    own = half_ref[: out_ref.shape[0], :]
    total = (kept_ref[...] + got_ref[...].astype(F32)).astype(BF16)
    first = project(own, weights_ref[0]) + project(total, weights_ref[1]) + biases_ref[4, 0:1, :]
    out_ref[...] = (
        own.astype(F32) + tail(first, weights_ref[2], biases_ref, gains_ref, 4)
    ).astype(BF16)


def swap(rows, axis, mask):
    return lax.ppermute(rows, axis, [(i, i ^ mask) for i in range(lax.axis_size(axis))])


def window_exchange(blocks, back):
    blk_count = lax.axis_size("blk")
    pieces = []
    for window in range(NEIGH):
        if blk_count == NEIGH:
            pieces.append(swap(blocks[window], "blk", window) if window else blocks[0])
        else:
            distance = window - NEIGH // 2
            distance = distance if back else -distance
            route = [((i - distance) % blk_count, i) for i in range(blk_count)]
            pieces.append(lax.ppermute(blocks[window], "blk", route) if distance else blocks[window])
    return pieces


def body(
    grid_nodes,
    enc_edges,
    enc_sender,
    enc_slot,
    enc_slot_node,
    mesh_nodes,
    mesh_edges,
    mesh_sender,
    mesh_receiver,
    mesh_send_node,
    grid_weights,
    enc_edge_weights,
    enc_node_weights,
    proc_edge_weights,
    proc_node_weights,
    biases,
    gains,
):
    blk_count, band_count = lax.axis_size("blk"), lax.axis_size("band")
    patch_rows, width = mesh_nodes.shape
    share_rows, half_rows = patch_rows // band_count, patch_rows // 2
    edge_rows, grid_rows, medge_rows = enc_edges.shape[0], grid_nodes.shape[0], mesh_edges.shape[0]
    slots = enc_slot_node.shape[1]
    cap = slots // NEIGH
    senders_all = mesh_send_node.shape[1]
    mcap = senders_all // blk_count
    for count in (blk_count, band_count, cap, mcap):
        assert count & (count - 1) == 0
    exact = blk_count == NEIGH
    unit = 2 * width * width
    piece = shape((cap, width), BF16)
    half_bf, half_f = shape((half_rows, width), BF16), shape((half_rows, width), F32)

    slot_keys = call(
        functools.partial(keys_kernel, exact),
        [piece] * NEIGH,
        (enc_slot_node, mesh_nodes, enc_edge_weights),
        [
            pltpu.VMEM((NEIGH, cap, width), BF16),
            pltpu.VMEM((patch_rows, width), BF16),
            pltpu.VMEM((width, width), BF16),
            pltpu.SemaphoreType.DMA((2,)),
        ],
        unit * 2 * slots,
        (1, 2),
    )
    keys = window_exchange(slot_keys, False)

    edge_part = call(
        edge_kernel,
        shape((edge_rows, width), F32),
        (enc_sender.reshape(1, edge_rows), grid_nodes, enc_edges, enc_edge_weights, biases),
        (),
        unit * 3 * edge_rows,
    )
    slot_sums = call(
        functools.partial(message_kernel, exact),
        [piece] * NEIGH,
        (enc_slot.reshape(1, edge_rows), edge_part, enc_edge_weights, biases, gains, *keys),
        [pltpu.VMEM((slots, width), BF16), pltpu.VMEM((edge_rows, width), BF16)],
        unit * 3 * edge_rows,
    )
    landed = window_exchange(slot_sums, True)

    grid_out = call(
        grid_kernel,
        shape((grid_rows, width), BF16),
        (grid_nodes, grid_weights, biases, gains),
        (),
        unit * 2 * grid_rows,
    )
    nodes_by_share = mesh_nodes.reshape(band_count, share_rows, width)
    node_part, mesh_part = call(
        functools.partial(early_kernel, band_count),
        [half_f, shape((medge_rows, width), F32)],
        (nodes_by_share, mesh_edges, enc_node_weights, proc_edge_weights, biases),
        (),
        unit * (half_rows + medge_rows),
    )

    given, kept = call(
        functools.partial(land_kernel, exact, band_count),
        [half_bf, half_f],
        (enc_slot_node, *landed),
        [pltpu.VMEM((NEIGH, cap, width), BF16)],
        unit * patch_rows,
    )
    got = swap(given, "band", 1)
    half = (kept + got.astype(F32)).astype(BF16)
    mask = 2
    while True:
        got = swap(half, "band", mask)
        if 2 * mask >= band_count:
            break
        half = crossed(half, got, share_rows, band_count, mask // 2)
        mask *= 2
    half_mid = call(
        functools.partial(node_kernel, band_count, mask // 2),
        half_bf,
        (half, got, nodes_by_share, node_part, enc_node_weights, biases, gains),
        (),
        unit * 2 * half_rows,
    )
    other_mid = swap(half_mid, "band", 1)

    half_blocks = shape((blk_count // 2, mcap, width), BF16)
    kept, given = call(
        functools.partial(sender_kernel, band_count),
        [half_blocks, half_blocks],
        (mesh_send_node, half_mid, other_mid, proc_edge_weights),
        [pltpu.VMEM((patch_rows, width), BF16), pltpu.VMEM((blk_count, mcap, width), BF16)],
        unit * 2 * senders_all,
    )
    mask = 1
    while True:
        got = swap(given, "blk", mask)
        senders = jnp.stack([kept, got.reshape(kept.shape)], axis=1)
        mask *= 2
        if mask == blk_count:
            break
        view = senders.reshape(blk_count // (2 * mask), 2, mask * mcap, width)
        kept, given = view[:, 0], view[:, 1]
    arrived_senders = senders.reshape(senders_all, width)
    receivers = mesh_receiver.reshape(1, medge_rows)

    mesh_part = call(
        functools.partial(target_kernel, band_count),
        shape((medge_rows, width), F32),
        (receivers, half_mid, other_mid, mesh_part, proc_edge_weights),
        [pltpu.VMEM((patch_rows, width), BF16)],
        unit * (patch_rows + medge_rows),
    )
    given, kept = call(
        functools.partial(process_kernel, band_count, mcap),
        [half_bf, half_f],
        (
            mesh_sender.reshape(1, medge_rows),
            receivers,
            mesh_part,
            arrived_senders,
            proc_edge_weights,
            biases,
            gains,
        ),
        [pltpu.VMEM((medge_rows, width), BF16)],
        unit * 3 * medge_rows,
    )
    got = swap(given, "band", 1)
    count = band_count // 2
    while count > 1:
        shares = kept + got.astype(F32)
        count //= 2
        kept, given = shares[: count * share_rows], shares[count * share_rows :].astype(BF16)
        got = swap(given, "band", 2 * count)
    mesh_out = call(
        last_kernel,
        shape((share_rows, width), BF16),
        (kept, got, half_mid, proc_node_weights, biases, gains),
        (),
        unit * 3 * share_rows,
    )
    return (grid_out, mesh_out)


def solution(mesh):
    rows = P(("blk", "band"), None)
    flat = P(("blk", "band"))
    in_specs = (rows, rows, flat, flat, rows, P("blk", None), rows, flat, flat, rows) + (P(),) * 7
    return jax.shard_map(
        body, mesh=mesh, in_specs=in_specs, out_specs=(rows, rows), check_vma=False
    )
```

```python
import functools

import jax
import jax.numpy as jnp
from jax import lax
from jax.experimental import pallas as pl
from jax.experimental.pallas import tpu as pltpu
from jax.sharding import PartitionSpec as P


NEIGH = 8
BF16 = jnp.bfloat16
F32 = jnp.float32
TILE = 256
GRANT = 16 << 20


def project(node_rows, weight):
    return jnp.dot(node_rows, weight, preferred_element_type=F32)


def silu(values):
    half = values * 0.5
    return half + half * jnp.tanh(half)


def normed(second, gain_row):
    center = second - jnp.mean(second, axis=-1, keepdims=True)
    spread = jnp.mean(center * center, axis=-1, keepdims=True)
    return center * (lax.rsqrt(spread + 1e-05) * gain_row)


def tail(first, weight, biases_ref, gains_ref, block):
    hidden = silu(first).astype(BF16)
    second = project(hidden, weight) + biases_ref[block, 1:2, :]
    return normed(second, gains_ref[block : block + 1, :])


def column(row):
    return jnp.broadcast_to(row, (128, row.shape[1])).T


def hot_columns(indices, names):
    wide = names.shape[1]
    if wide <= 128:
        return (indices[:, :wide] == names).astype(F32).astype(BF16)
    parts = [
        (indices == names[:, at : at + 128]).astype(F32).astype(BF16) for at in range(0, wide, 128)
    ]
    return jnp.concatenate(parts, axis=1)


def hot_rows(row, names):
    return (row == names).astype(F32).astype(BF16)


def lanes(count):
    return lax.broadcasted_iota(jnp.int32, (1, count), 1)


def sublanes(count):
    return lax.broadcasted_iota(jnp.int32, (count, 1), 0)


def share_names(iota, share_rows, band_count, core):
    half_count = band_count // 2
    x = lax.div(lax.axis_index("band"), 2)
    names = iota
    for place in range(band_count):
        share = 2 * ((place % half_count) ^ x) + (core if place < half_count else 1 - core)
        offset = (share - place) * share_rows
        inside = (iota >= place * share_rows) & (iota < (place + 1) * share_rows)
        names = jnp.where(inside, iota + offset, names)
    return names


def call(kernel, outs, args, scratch=(), flops=0, in_hbm=()):
    single = not isinstance(outs, (list, tuple))
    outs = [outs] if single else outs
    vmem = pl.BlockSpec(memory_space=pltpu.VMEM)
    args = [
        pltpu.with_memory_space_constraint(arg, pltpu.HBM if at in in_hbm else pltpu.VMEM)
        for at, arg in enumerate(args)
    ]
    results = pl.pallas_call(
        kernel,
        out_shape=tuple(pltpu.VMEM(out.shape, out.dtype) for out in outs),
        in_specs=[
            pl.BlockSpec(memory_space=pltpu.HBM) if at in in_hbm else vmem for at in range(len(args))
        ],
        out_specs=(vmem,) * len(outs),
        scratch_shapes=list(scratch),
        cost_estimate=pl.CostEstimate(flops=flops, transcendentals=0, bytes_accessed=0),
        compiler_params=pltpu.CompilerParams(vmem_limit_bytes=GRANT),
    )(*args)
    return results[0] if single else results


def shape(dims, kind):
    return jax.ShapeDtypeStruct(dims, kind)


def window_of(mask, exact):
    if not exact:
        return mask
    blk = lax.axis_index("blk")
    return lax.rem(blk - (blk ^ mask) + NEIGH // 2 + NEIGH, NEIGH)


def keys_kernel(exact, node_hbm, mesh_hbm, weights_hbm, *refs):
    outs, (held, nodes, mesh, weight, sems) = refs[:NEIGH], refs[NEIGH:]
    copies = [
        pltpu.make_async_copy(source, target, sems.at[at])
        for at, (source, target) in enumerate(
            ((node_hbm, nodes), (mesh_hbm, mesh), (weights_hbm.at[2], weight))
        )
    ]
    for copy in copies:
        copy.start()
    copies[0].wait()
    picks = hot_columns(column(nodes[...]), lanes(mesh.shape[0]))
    copies[1].wait()
    rows = project(picks, mesh[...]).astype(BF16)
    copies[2].wait()
    keys = project(rows, weight[...]).astype(BF16)
    held[...] = keys.reshape(held.shape)
    for mask in range(NEIGH):
        outs[mask][...] = held[window_of(mask, exact)]


def edge_kernel(sender_ref, grid_ref, edges_ref, weights_ref, biases_ref, part_ref):
    names = lanes(grid_ref.shape[0])
    senders = column(sender_ref[...])
    for at in range(0, edges_ref.shape[0], TILE):
        picks = hot_columns(senders[at : at + TILE], names)
        nodes = project(picks, grid_ref[...]).astype(BF16)
        part_ref[at : at + TILE, :] = (
            project(edges_ref[at : at + TILE, :], weights_ref[0])
            + project(nodes, weights_ref[1])
            + biases_ref[1, 0:1, :]
        )


def grid_kernel(grid_ref, weights_ref, biases_ref, gains_ref, out_ref):
    for at in range(0, grid_ref.shape[0], TILE):
        nodes = grid_ref[at : at + TILE, :]
        first = project(nodes, weights_ref[0]) + biases_ref[0, 0:1, :]
        out_ref[at : at + TILE, :] = (
            nodes.astype(F32) + tail(first, weights_ref[1], biases_ref, gains_ref, 0)
        ).astype(BF16)


def message_kernel(exact, slot_ref, part_ref, weights_ref, biases_ref, gains_ref, near_ref, far_ref, *refs):
    keys, outs, (lists_ref, table, sent) = refs[:NEIGH], refs[NEIGH : 2 * NEIGH], refs[2 * NEIGH :]
    lists_ref[: near_ref.shape[0], :] = near_ref[...]
    lists_ref[near_ref.shape[0] :, :] = far_ref[...]
    cap = keys[0].shape[0]
    for window in range(NEIGH):
        table[window * cap : (window + 1) * cap, :] = keys[window][...]
    row = slot_ref[...]
    if exact:
        blk = lax.axis_index("blk")
        patch = (lax.div(row, cap) + (blk + NEIGH // 2)) & (NEIGH - 1)
        row = (patch ^ blk) * cap + lax.rem(row, cap)
    slots = column(row)
    names = lanes(table.shape[0])
    for at in range(0, part_ref.shape[0], TILE):
        picks = hot_columns(slots[at : at + TILE], names)
        first = part_ref[at : at + TILE, :] + project(picks, table[...])
        sent[at : at + TILE, :] = tail(first, weights_ref[3], biases_ref, gains_ref, 1).astype(BF16)
    sums = project(hot_rows(row, sublanes(table.shape[0])), sent[...]).astype(BF16)
    for window in range(NEIGH):
        outs[window][...] = sums[window * cap : (window + 1) * cap, :]


def hot_lists(lists_ref, row):
    return jnp.concatenate(
        [
            hot_columns(column(lists_ref[at : at + 1, :]), row)
            for at in range(lists_ref.shape[0])
        ],
        axis=0,
    )


def land_kernel(exact, band_count, node_ref, own_ref, other_ref, *refs):
    pieces, (given_ref, kept_ref, listed_ref, held) = refs[:NEIGH], refs[NEIGH:]
    for mask in range(NEIGH):
        held[window_of(mask, exact)] = pieces[mask][...]
    half = kept_ref.shape[0]
    core = lax.rem(lax.axis_index("band"), 2)
    names = share_names(sublanes(2 * half), 2 * half // band_count, band_count, 1 - core)
    row = node_ref[...]
    landed = held[...].reshape(-1, held.shape[2])
    given_ref[:half, :] = project(hot_rows(row, names[:half]), landed).astype(BF16)
    given_ref[half:, :] = project(hot_lists(other_ref, row), landed).astype(BF16)
    kept_ref[...] = project(hot_rows(row, names[half:]), landed)
    listed_ref[...] = project(hot_lists(own_ref, row), landed)


def own_share(place):
    band = lax.axis_index("band")
    return 2 * (place ^ lax.div(band, 2)) + lax.rem(band, 2)


def early_kernel(
    band_count, send_ref, nodes_ref, edges_ref, w_nodes, w_edges, biases_ref, node_part_ref, edge_part_ref, listed_ref, listed_part_ref
):
    share = node_part_ref.shape[0] // (band_count // 2)
    nodes = nodes_ref[...].reshape(-1, nodes_ref.shape[2])
    rows = project(hot_columns(column(send_ref[...]), lanes(nodes.shape[0])), nodes).astype(BF16)
    listed_ref[...] = rows
    listed_part_ref[...] = project(rows, w_nodes[0]) + biases_ref[2, 0:1, :]
    for place in range(band_count // 2):
        node_part_ref[place * share : (place + 1) * share, :] = (
            project(nodes_ref[own_share(place)], w_nodes[0]) + biases_ref[2, 0:1, :]
        )
    for at in range(0, edges_ref.shape[0], TILE):
        edge_part_ref[at : at + TILE, :] = (
            project(edges_ref[at : at + TILE, :], w_edges[0]) + biases_ref[3, 0:1, :]
        )


def node_kernel(band_count, bit, half_ref, got_ref, nodes_ref, part_ref, weights_ref, biases_ref, gains_ref, out_ref):
    share = out_ref.shape[0] // (band_count // 2)
    total = crossed(half_ref, got_ref, share, band_count, bit)
    first = part_ref[...] + project(total, weights_ref[1])
    change = tail(first, weights_ref[2], biases_ref, gains_ref, 2)
    for place in range(band_count // 2):
        at = place * share
        out_ref[at : at + share, :] = (
            nodes_ref[own_share(place)].astype(F32) + change[at : at + share, :]
        ).astype(BF16)


def crossed(half, got, share, band_count, bit):
    parts = []
    for place in range(band_count // 2):
        at, other = place * share, (place ^ bit) * share
        parts.append(half[at : at + share, :].astype(F32) + got[other : other + share, :].astype(F32))
    return jnp.concatenate(parts, axis=0).astype(BF16)


def sender_kernel(
    sums_ref, got_ref, nodes_ref, part_ref, w_nodes, w_edges, biases_ref, gains_ref, kept_ref, given_ref, held
):
    total = (sums_ref[...].astype(F32) + got_ref[...].astype(F32)).astype(BF16)
    first = part_ref[...] + project(total, w_nodes[1])
    change = tail(first, w_nodes[2], biases_ref, gains_ref, 2)
    rows = (nodes_ref[...].astype(F32) + change).astype(BF16)
    held[...] = project(rows, w_edges[1]).astype(BF16).reshape(held.shape)
    blk = lax.axis_index("blk")
    for pair in range(kept_ref.shape[0]):
        kept_ref[pair] = held[blk ^ (2 * pair)]
        given_ref[pair] = held[blk ^ (2 * pair + 1)]


def target_kernel(band_count, receiver_ref, own_ref, other_ref, part_ref, weights_ref, out_ref, table):
    half = own_ref.shape[0]
    table[:half, :] = project(own_ref[...], weights_ref[2]).astype(BF16)
    table[half:, :] = project(other_ref[...], weights_ref[2]).astype(BF16)
    core = lax.rem(lax.axis_index("band"), 2)
    names = share_names(lanes(2 * half), 2 * half // band_count, band_count, core)
    receivers = column(receiver_ref[...])
    for at in range(0, part_ref.shape[0], TILE):
        picks = hot_columns(receivers[at : at + TILE], names)
        out_ref[at : at + TILE, :] = part_ref[at : at + TILE, :] + project(picks, table[...])


def process_kernel(
    band_count, mcap, sender_ref, receiver_ref, part_ref, keys_ref, weights_ref, biases_ref, gains_ref, given_ref, kept_ref, sent
):
    senders = column(sender_ref[...] ^ (lax.axis_index("blk") * mcap))
    names = lanes(keys_ref.shape[0])
    for at in range(0, part_ref.shape[0], TILE):
        picks = hot_columns(senders[at : at + TILE], names)
        first = part_ref[at : at + TILE, :] + project(picks, keys_ref[...])
        sent[at : at + TILE, :] = tail(first, weights_ref[3], biases_ref, gains_ref, 3).astype(BF16)
    half = given_ref.shape[0]
    core = lax.rem(lax.axis_index("band"), 2)
    places = share_names(sublanes(2 * half), 2 * half // band_count, band_count, 1 - core)
    given_ref[...] = project(hot_rows(receiver_ref[...], places[:half]), sent[...]).astype(BF16)
    kept_ref[...] = project(hot_rows(receiver_ref[...], places[half:]), sent[...])


def last_kernel(kept_ref, got_ref, half_ref, weights_ref, biases_ref, gains_ref, out_ref):
    own = half_ref[: out_ref.shape[0], :]
    total = (kept_ref[...] + got_ref[...].astype(F32)).astype(BF16)
    first = project(own, weights_ref[0]) + project(total, weights_ref[1]) + biases_ref[4, 0:1, :]
    out_ref[...] = (
        own.astype(F32) + tail(first, weights_ref[2], biases_ref, gains_ref, 4)
    ).astype(BF16)


def swap(rows, axis, mask):
    return lax.ppermute(rows, axis, [(i, i ^ mask) for i in range(lax.axis_size(axis))])


def window_exchange(blocks, back):
    blk_count = lax.axis_size("blk")
    pieces = []
    for window in range(NEIGH):
        if blk_count == NEIGH:
            pieces.append(swap(blocks[window], "blk", window) if window else blocks[0])
        else:
            distance = window - NEIGH // 2
            distance = distance if back else -distance
            route = [((i - distance) % blk_count, i) for i in range(blk_count)]
            pieces.append(lax.ppermute(blocks[window], "blk", route) if distance else blocks[window])
    return pieces


def body(
    grid_nodes,
    enc_edges,
    enc_sender,
    enc_slot,
    enc_slot_node,
    mesh_nodes,
    mesh_edges,
    mesh_sender,
    mesh_receiver,
    mesh_send_node,
    grid_weights,
    enc_edge_weights,
    enc_node_weights,
    proc_edge_weights,
    proc_node_weights,
    biases,
    gains,
):
    blk_count, band_count = lax.axis_size("blk"), lax.axis_size("band")
    patch_rows, width = mesh_nodes.shape
    share_rows, half_rows = patch_rows // band_count, patch_rows // 2
    edge_rows, grid_rows, medge_rows = enc_edges.shape[0], grid_nodes.shape[0], mesh_edges.shape[0]
    slots = enc_slot_node.shape[1]
    cap = slots // NEIGH
    senders_all = mesh_send_node.shape[1]
    mcap = senders_all // blk_count
    for count in (blk_count, band_count, cap, mcap):
        assert count & (count - 1) == 0
    exact = blk_count == NEIGH
    unit = 2 * width * width
    piece = shape((cap, width), BF16)
    half_bf, half_f = shape((half_rows, width), BF16), shape((half_rows, width), F32)

    slot_keys = call(
        functools.partial(keys_kernel, exact),
        [piece] * NEIGH,
        (enc_slot_node, mesh_nodes, enc_edge_weights),
        [
            pltpu.VMEM((NEIGH, cap, width), BF16),
            pltpu.VMEM((1, slots), jnp.int32),
            pltpu.VMEM((patch_rows, width), BF16),
            pltpu.VMEM((width, width), BF16),
            pltpu.SemaphoreType.DMA((3,)),
        ],
        unit * 2 * slots,
        (0, 1, 2),
    )
    keys = window_exchange(slot_keys, False)

    edge_part = call(
        edge_kernel,
        shape((edge_rows, width), F32),
        (enc_sender.reshape(1, edge_rows), grid_nodes, enc_edges, enc_edge_weights, biases),
        (),
        unit * 3 * edge_rows,
    )
    near, mask = mesh_send_node, 2
    while True:
        far = swap(near, "band", mask)
        mask *= 2
        if mask >= band_count:
            break
        near = jnp.concatenate([near, far], axis=0)
    *slot_sums, lists = call(
        functools.partial(message_kernel, exact),
        [piece] * NEIGH + [shape((band_count // 2, senders_all), jnp.int32)],
        (enc_slot.reshape(1, edge_rows), edge_part, enc_edge_weights, biases, gains, near, far, *keys),
        [pltpu.VMEM((slots, width), BF16), pltpu.VMEM((edge_rows, width), BF16)],
        unit * 3 * edge_rows,
    )
    landed = window_exchange(slot_sums, True)

    grid_out = call(
        grid_kernel,
        shape((grid_rows, width), BF16),
        (grid_nodes, grid_weights, biases, gains),
        (),
        unit * 2 * grid_rows,
    )
    other_lists = swap(lists, "band", 1)
    listed = band_count // 2 * senders_all

    nodes_by_share = mesh_nodes.reshape(band_count, share_rows, width)
    node_part, mesh_part, listed_nodes, listed_part = call(
        functools.partial(early_kernel, band_count),
        [half_f, shape((medge_rows, width), F32), shape((senders_all, width), BF16), shape((senders_all, width), F32)],
        (mesh_send_node, nodes_by_share, mesh_edges, enc_node_weights, proc_edge_weights, biases),
        (),
        unit * (half_rows + medge_rows + 2 * senders_all),
    )

    given, kept, kept_listed = call(
        functools.partial(land_kernel, exact, band_count),
        [shape((half_rows + listed, width), BF16), half_f, shape((listed, width), F32)],
        (enc_slot_node, lists, other_lists, *landed),
        [pltpu.VMEM((NEIGH, cap, width), BF16)],
        unit * (patch_rows + 2 * listed),
    )
    got = swap(given, "band", 1)
    half = (kept + got[:half_rows].astype(F32)).astype(BF16)
    sums = (kept_listed + got[half_rows:].astype(F32)).astype(BF16)
    count = band_count // 2
    while True:
        count //= 2
        kept, given = sums[: count * senders_all], sums[count * senders_all :]
        got_listed = swap(given, "band", 2 * count)
        if count == 1:
            break
        sums = (kept.astype(F32) + got_listed.astype(F32)).astype(BF16)
    mask = 2
    while True:
        got = swap(half, "band", mask)
        if 2 * mask >= band_count:
            break
        half = crossed(half, got, share_rows, band_count, mask // 2)
        mask *= 2

    half_blocks = shape((blk_count // 2, mcap, width), BF16)
    kept, given = call(
        sender_kernel,
        [half_blocks, half_blocks],
        (
            kept,
            got_listed,
            listed_nodes,
            listed_part,
            enc_node_weights,
            proc_edge_weights,
            biases,
            gains,
        ),
        [pltpu.VMEM((blk_count, mcap, width), BF16)],
        unit * 3 * senders_all,
    )
    bit = 1
    while True:
        got_rows = swap(given, "blk", bit)
        senders = jnp.stack([kept, got_rows.reshape(kept.shape)], axis=1)
        bit *= 2
        if bit == blk_count:
            break
        view = senders.reshape(blk_count // (2 * bit), 2, bit * mcap, width)
        kept, given = view[:, 0], view[:, 1]
    arrived_senders = senders.reshape(senders_all, width)
    receivers = mesh_receiver.reshape(1, medge_rows)

    half_mid = call(
        functools.partial(node_kernel, band_count, mask // 2),
        half_bf,
        (half, got, nodes_by_share, node_part, enc_node_weights, biases, gains),
        (),
        unit * 2 * half_rows,
    )
    other_mid = swap(half_mid, "band", 1)

    mesh_part = call(
        functools.partial(target_kernel, band_count),
        shape((medge_rows, width), F32),
        (receivers, half_mid, other_mid, mesh_part, proc_edge_weights),
        [pltpu.VMEM((patch_rows, width), BF16)],
        unit * (patch_rows + medge_rows),
    )
    given, kept = call(
        functools.partial(process_kernel, band_count, mcap),
        [half_bf, half_f],
        (
            mesh_sender.reshape(1, medge_rows),
            receivers,
            mesh_part,
            arrived_senders,
            proc_edge_weights,
            biases,
            gains,
        ),
        [pltpu.VMEM((medge_rows, width), BF16)],
        unit * 3 * medge_rows,
    )
    got = swap(given, "band", 1)
    count = band_count // 2
    while count > 1:
        shares = kept + got.astype(F32)
        count //= 2
        kept, given = shares[: count * share_rows], shares[count * share_rows :].astype(BF16)
        got = swap(given, "band", 2 * count)
    mesh_out = call(
        last_kernel,
        shape((share_rows, width), BF16),
        (kept, got, half_mid, proc_node_weights, biases, gains),
        (),
        unit * 3 * share_rows,
    )
    return (grid_out, mesh_out)


def solution(mesh):
    rows = P(("blk", "band"), None)
    flat = P(("blk", "band"))
    in_specs = (rows, rows, flat, flat, rows, P("blk", None), rows, flat, flat, rows) + (P(),) * 7
    return jax.shard_map(body, mesh=mesh, in_specs=in_specs, out_specs=(rows, rows), check_vma=False)
```

```python
import functools

import jax
import jax.numpy as jnp
from jax import lax
from jax.experimental import pallas as pl
from jax.experimental.pallas import tpu as pltpu
from jax.sharding import PartitionSpec as P


NEIGH = 8
BF16 = jnp.bfloat16
F32 = jnp.float32
TILE = 256
GRANT = 16 << 20


def project(node_rows, weight):
    return jnp.dot(node_rows, weight, preferred_element_type=F32)


def silu(values):
    half = values * 0.5
    return half + half * jnp.tanh(half)


def normed(second, gain_row):
    center = second - jnp.mean(second, axis=-1, keepdims=True)
    spread = jnp.mean(center * center, axis=-1, keepdims=True)
    return center * (lax.rsqrt(spread + 1e-05) * gain_row)


def tail(first, weight, biases_ref, gains_ref, block):
    hidden = silu(first).astype(BF16)
    second = project(hidden, weight) + biases_ref[block, 1:2, :]
    return normed(second, gains_ref[block : block + 1, :])


def column(row):
    return jnp.broadcast_to(row, (128, row.shape[1])).T


def hot_columns(indices, names):
    wide = names.shape[1]
    if wide <= 128:
        return (indices[:, :wide] == names).astype(F32).astype(BF16)
    parts = [
        (indices == names[:, at : at + 128]).astype(F32).astype(BF16) for at in range(0, wide, 128)
    ]
    return jnp.concatenate(parts, axis=1)


def hot_rows(row, names):
    return (row == names).astype(F32).astype(BF16)


def lanes(count):
    return lax.broadcasted_iota(jnp.int32, (1, count), 1)


def sublanes(count):
    return lax.broadcasted_iota(jnp.int32, (count, 1), 0)


def share_names(iota, share_rows, band_count, core):
    half_count = band_count // 2
    x = lax.div(lax.axis_index("band"), 2)
    names = iota
    for place in range(band_count):
        share = 2 * ((place % half_count) ^ x) + (core if place < half_count else 1 - core)
        offset = (share - place) * share_rows
        inside = (iota >= place * share_rows) & (iota < (place + 1) * share_rows)
        names = jnp.where(inside, iota + offset, names)
    return names


def call(kernel, outs, args, scratch=(), flops=0, in_hbm=()):
    single = not isinstance(outs, (list, tuple))
    outs = [outs] if single else outs
    vmem = pl.BlockSpec(memory_space=pltpu.VMEM)
    args = [
        pltpu.with_memory_space_constraint(arg, pltpu.HBM if at in in_hbm else pltpu.VMEM)
        for at, arg in enumerate(args)
    ]
    results = pl.pallas_call(
        kernel,
        out_shape=tuple(pltpu.VMEM(out.shape, out.dtype) for out in outs),
        in_specs=[
            pl.BlockSpec(memory_space=pltpu.HBM) if at in in_hbm else vmem for at in range(len(args))
        ],
        out_specs=(vmem,) * len(outs),
        scratch_shapes=list(scratch),
        cost_estimate=pl.CostEstimate(flops=flops, transcendentals=0, bytes_accessed=0),
        compiler_params=pltpu.CompilerParams(vmem_limit_bytes=GRANT),
    )(*args)
    return results[0] if single else results


def shape(dims, kind):
    return jax.ShapeDtypeStruct(dims, kind)


def window_of(mask, exact):
    if not exact:
        return mask
    blk = lax.axis_index("blk")
    return lax.rem(blk - (blk ^ mask) + NEIGH // 2 + NEIGH, NEIGH)


def keys_kernel(exact, node_hbm, mesh_hbm, weights_hbm, *refs):
    outs, (held, nodes, mesh, weight, sems) = refs[:NEIGH], refs[NEIGH:]
    copies = [
        pltpu.make_async_copy(source, target, sems.at[at])
        for at, (source, target) in enumerate(
            ((node_hbm, nodes), (mesh_hbm, mesh), (weights_hbm.at[2], weight))
        )
    ]
    for copy in copies:
        copy.start()
    copies[0].wait()
    picks = hot_columns(column(nodes[...]), lanes(mesh.shape[0]))
    copies[1].wait()
    rows = project(picks, mesh[...]).astype(BF16)
    copies[2].wait()
    keys = project(rows, weight[...]).astype(BF16)
    held[...] = keys.reshape(held.shape)
    for mask in range(NEIGH):
        outs[mask][...] = held[window_of(mask, exact)]


def edge_kernel(sender_ref, grid_ref, weights_ref, biases_ref, edges_hbm, part_ref, edges, sems):
    tiles = range(0, edges.shape[0], TILE)
    copies = [
        pltpu.make_async_copy(
            edges_hbm.at[pl.ds(at, TILE), :], edges.at[pl.ds(at, TILE), :], sems.at[at // TILE]
        )
        for at in tiles
    ]
    for copy in copies:
        copy.start()
    names = lanes(grid_ref.shape[0])
    senders = column(sender_ref[...])
    for at, copy in zip(tiles, copies):
        picks = hot_columns(senders[at : at + TILE], names)
        nodes = project(picks, grid_ref[...]).astype(BF16)
        part = project(nodes, weights_ref[1]) + biases_ref[1, 0:1, :]
        copy.wait()
        part_ref[at : at + TILE, :] = part + project(edges[at : at + TILE, :], weights_ref[0])


def grid_kernel(grid_ref, weights_ref, biases_ref, gains_ref, out_ref):
    for at in range(0, grid_ref.shape[0], TILE):
        nodes = grid_ref[at : at + TILE, :]
        first = project(nodes, weights_ref[0]) + biases_ref[0, 0:1, :]
        out_ref[at : at + TILE, :] = (
            nodes.astype(F32) + tail(first, weights_ref[1], biases_ref, gains_ref, 0)
        ).astype(BF16)


def message_kernel(exact, slot_ref, part_ref, weights_ref, biases_ref, gains_ref, near_ref, far_ref, *refs):
    keys, outs, (lists_ref, table, sent) = refs[:NEIGH], refs[NEIGH : 2 * NEIGH], refs[2 * NEIGH :]
    lists_ref[: near_ref.shape[0], :] = near_ref[...]
    lists_ref[near_ref.shape[0] :, :] = far_ref[...]
    cap = keys[0].shape[0]
    for window in range(NEIGH):
        table[window * cap : (window + 1) * cap, :] = keys[window][...]
    row = slot_ref[...]
    if exact:
        blk = lax.axis_index("blk")
        patch = (lax.div(row, cap) + (blk + NEIGH // 2)) & (NEIGH - 1)
        row = (patch ^ blk) * cap + lax.rem(row, cap)
    slots = column(row)
    names = lanes(table.shape[0])
    for at in range(0, part_ref.shape[0], TILE):
        picks = hot_columns(slots[at : at + TILE], names)
        first = part_ref[at : at + TILE, :] + project(picks, table[...])
        sent[at : at + TILE, :] = tail(first, weights_ref[3], biases_ref, gains_ref, 1).astype(BF16)
    sums = project(hot_rows(row, sublanes(table.shape[0])), sent[...]).astype(BF16)
    for window in range(NEIGH):
        outs[window][...] = sums[window * cap : (window + 1) * cap, :]


def hot_lists(lists_ref, row):
    return jnp.concatenate(
        [
            hot_columns(column(lists_ref[at : at + 1, :]), row)
            for at in range(lists_ref.shape[0])
        ],
        axis=0,
    )


def land_kernel(exact, band_count, half, node_ref, lists_ref, *refs):
    pieces, (given_ref, held) = refs[:NEIGH], refs[NEIGH:]
    for mask in range(NEIGH):
        held[window_of(mask, exact)] = pieces[mask][...]
    core = lax.rem(lax.axis_index("band"), 2)
    names = share_names(sublanes(2 * half), 2 * half // band_count, band_count, 1 - core)
    row = node_ref[...]
    landed = held[...].reshape(-1, held.shape[2])
    given_ref[:half, :] = project(hot_rows(row, names[:half]), landed).astype(BF16)
    given_ref[half:, :] = project(hot_lists(lists_ref, row), landed).astype(BF16)


def keep_kernel(band_count, node_ref, lists_ref, held, kept_ref, listed_ref):
    half = kept_ref.shape[0]
    core = lax.rem(lax.axis_index("band"), 2)
    names = share_names(sublanes(2 * half), 2 * half // band_count, band_count, core)
    row = node_ref[...]
    landed = held[...].reshape(-1, held.shape[2])
    kept_ref[...] = project(hot_rows(row, names[:half]), landed)
    listed_ref[...] = project(hot_lists(lists_ref, row), landed)


def own_share(place):
    band = lax.axis_index("band")
    return 2 * (place ^ lax.div(band, 2)) + lax.rem(band, 2)


def early_kernel(
    band_count, send_ref, nodes_ref, edges_ref, w_nodes, w_edges, biases_ref, node_part_ref, edge_part_ref, listed_ref, listed_part_ref
):
    share = node_part_ref.shape[0] // (band_count // 2)
    nodes = nodes_ref[...].reshape(-1, nodes_ref.shape[2])
    rows = project(hot_columns(column(send_ref[...]), lanes(nodes.shape[0])), nodes).astype(BF16)
    listed_ref[...] = rows
    listed_part_ref[...] = project(rows, w_nodes[0]) + biases_ref[2, 0:1, :]
    for place in range(band_count // 2):
        node_part_ref[place * share : (place + 1) * share, :] = (
            project(nodes_ref[own_share(place)], w_nodes[0]) + biases_ref[2, 0:1, :]
        )
    for at in range(0, edges_ref.shape[0], TILE):
        edge_part_ref[at : at + TILE, :] = (
            project(edges_ref[at : at + TILE, :], w_edges[0]) + biases_ref[3, 0:1, :]
        )


def node_kernel(band_count, bit, half_ref, got_ref, nodes_ref, part_ref, weights_ref, biases_ref, gains_ref, out_ref):
    share = out_ref.shape[0] // (band_count // 2)
    total = crossed(half_ref, got_ref, share, band_count, bit)
    first = part_ref[...] + project(total, weights_ref[1])
    change = tail(first, weights_ref[2], biases_ref, gains_ref, 2)
    for place in range(band_count // 2):
        at = place * share
        out_ref[at : at + share, :] = (
            nodes_ref[own_share(place)].astype(F32) + change[at : at + share, :]
        ).astype(BF16)


def crossed(half, got, share, band_count, bit):
    parts = []
    for place in range(band_count // 2):
        at, other = place * share, (place ^ bit) * share
        parts.append(half[at : at + share, :].astype(F32) + got[other : other + share, :].astype(F32))
    return jnp.concatenate(parts, axis=0).astype(BF16)


def sender_kernel(
    sums_ref, got_ref, nodes_ref, part_ref, w_nodes, w_edges, biases_ref, gains_ref, kept_ref, given_ref, held
):
    total = (sums_ref[...].astype(F32) + got_ref[...].astype(F32)).astype(BF16)
    first = part_ref[...] + project(total, w_nodes[1])
    change = tail(first, w_nodes[2], biases_ref, gains_ref, 2)
    rows = (nodes_ref[...].astype(F32) + change).astype(BF16)
    held[...] = project(rows, w_edges[1]).astype(BF16).reshape(held.shape)
    blk = lax.axis_index("blk")
    for pair in range(kept_ref.shape[0]):
        kept_ref[pair] = held[blk ^ (2 * pair)]
        given_ref[pair] = held[blk ^ (2 * pair + 1)]


def target_kernel(band_count, receiver_ref, own_ref, other_ref, part_ref, weights_ref, out_ref, table):
    half = own_ref.shape[0]
    table[:half, :] = project(own_ref[...], weights_ref[2]).astype(BF16)
    table[half:, :] = project(other_ref[...], weights_ref[2]).astype(BF16)
    core = lax.rem(lax.axis_index("band"), 2)
    names = share_names(lanes(2 * half), 2 * half // band_count, band_count, core)
    receivers = column(receiver_ref[...])
    for at in range(0, part_ref.shape[0], TILE):
        picks = hot_columns(receivers[at : at + TILE], names)
        out_ref[at : at + TILE, :] = part_ref[at : at + TILE, :] + project(picks, table[...])


def process_kernel(
    band_count, mcap, sender_ref, receiver_ref, part_ref, keys_ref, weights_ref, biases_ref, gains_ref, given_ref, sent
):
    senders = column(sender_ref[...] ^ (lax.axis_index("blk") * mcap))
    names = lanes(keys_ref.shape[0])
    for at in range(0, part_ref.shape[0], TILE):
        picks = hot_columns(senders[at : at + TILE], names)
        first = part_ref[at : at + TILE, :] + project(picks, keys_ref[...])
        sent[at : at + TILE, :] = tail(first, weights_ref[3], biases_ref, gains_ref, 3).astype(BF16)
    half = given_ref.shape[0]
    core = lax.rem(lax.axis_index("band"), 2)
    places = share_names(sublanes(2 * half), 2 * half // band_count, band_count, 1 - core)
    given_ref[...] = project(hot_rows(receiver_ref[...], places[:half]), sent[...]).astype(BF16)


def own_kernel(band_count, receiver_ref, sent_ref, half_ref, weights_ref, biases_ref, kept_ref, part_ref):
    half = kept_ref.shape[0]
    core = lax.rem(lax.axis_index("band"), 2)
    places = share_names(sublanes(2 * half), 2 * half // band_count, band_count, core)
    kept_ref[...] = project(hot_rows(receiver_ref[...], places[:half]), sent_ref[...])
    part_ref[...] = project(half_ref[: part_ref.shape[0], :], weights_ref[0]) + biases_ref[4, 0:1, :]


def last_kernel(kept_ref, got_ref, half_ref, part_ref, weights_ref, biases_ref, gains_ref, out_ref):
    own = half_ref[: out_ref.shape[0], :]
    total = (kept_ref[...] + got_ref[...].astype(F32)).astype(BF16)
    first = part_ref[...] + project(total, weights_ref[1])
    out_ref[...] = (
        own.astype(F32) + tail(first, weights_ref[2], biases_ref, gains_ref, 4)
    ).astype(BF16)


def swap(rows, axis, mask):
    return lax.ppermute(rows, axis, [(i, i ^ mask) for i in range(lax.axis_size(axis))])


def window_exchange(blocks, back):
    blk_count = lax.axis_size("blk")
    pieces = []
    for window in range(NEIGH):
        if blk_count == NEIGH:
            pieces.append(swap(blocks[window], "blk", window) if window else blocks[0])
        else:
            distance = window - NEIGH // 2
            distance = distance if back else -distance
            route = [((i - distance) % blk_count, i) for i in range(blk_count)]
            pieces.append(lax.ppermute(blocks[window], "blk", route) if distance else blocks[window])
    return pieces


def body(
    grid_nodes,
    enc_edges,
    enc_sender,
    enc_slot,
    enc_slot_node,
    mesh_nodes,
    mesh_edges,
    mesh_sender,
    mesh_receiver,
    mesh_send_node,
    grid_weights,
    enc_edge_weights,
    enc_node_weights,
    proc_edge_weights,
    proc_node_weights,
    biases,
    gains,
):
    blk_count, band_count = lax.axis_size("blk"), lax.axis_size("band")
    patch_rows, width = mesh_nodes.shape
    share_rows, half_rows = patch_rows // band_count, patch_rows // 2
    edge_rows, grid_rows, medge_rows = enc_edges.shape[0], grid_nodes.shape[0], mesh_edges.shape[0]
    slots = enc_slot_node.shape[1]
    cap = slots // NEIGH
    senders_all = mesh_send_node.shape[1]
    mcap = senders_all // blk_count
    for count in (blk_count, band_count, cap, mcap):
        assert count & (count - 1) == 0
    exact = blk_count == NEIGH
    unit = 2 * width * width
    piece = shape((cap, width), BF16)
    half_bf, half_f = shape((half_rows, width), BF16), shape((half_rows, width), F32)

    slot_keys = call(
        functools.partial(keys_kernel, exact),
        [piece] * NEIGH,
        (enc_slot_node, mesh_nodes, enc_edge_weights),
        [
            pltpu.VMEM((NEIGH, cap, width), BF16),
            pltpu.VMEM((1, slots), jnp.int32),
            pltpu.VMEM((patch_rows, width), BF16),
            pltpu.VMEM((width, width), BF16),
            pltpu.SemaphoreType.DMA((3,)),
        ],
        unit * 2 * slots,
        (0, 1, 2),
    )
    keys = window_exchange(slot_keys, False)

    edge_part = call(
        edge_kernel,
        shape((edge_rows, width), F32),
        (enc_sender.reshape(1, edge_rows), grid_nodes, enc_edge_weights, biases, enc_edges),
        [pltpu.VMEM((edge_rows, width), BF16), pltpu.SemaphoreType.DMA((edge_rows // TILE,))],
        unit * 3 * edge_rows,
        (4,),
    )
    near, mask = mesh_send_node, 2
    while True:
        far = swap(near, "band", mask)
        mask *= 2
        if mask >= band_count:
            break
        near = jnp.concatenate([near, far], axis=0)
    *slot_sums, lists = call(
        functools.partial(message_kernel, exact),
        [piece] * NEIGH + [shape((band_count // 2, senders_all), jnp.int32)],
        (enc_slot.reshape(1, edge_rows), edge_part, enc_edge_weights, biases, gains, near, far, *keys),
        [pltpu.VMEM((slots, width), BF16), pltpu.VMEM((edge_rows, width), BF16)],
        unit * 3 * edge_rows,
    )
    landed = window_exchange(slot_sums, True)

    grid_out = call(
        grid_kernel,
        shape((grid_rows, width), BF16),
        (grid_nodes, grid_weights, biases, gains),
        (),
        unit * 2 * grid_rows,
    )
    other_lists = swap(lists, "band", 1)
    listed = band_count // 2 * senders_all

    nodes_by_share = mesh_nodes.reshape(band_count, share_rows, width)
    node_part, mesh_part, listed_nodes, listed_part = call(
        functools.partial(early_kernel, band_count),
        [half_f, shape((medge_rows, width), F32), shape((senders_all, width), BF16), shape((senders_all, width), F32)],
        (mesh_send_node, nodes_by_share, mesh_edges, enc_node_weights, proc_edge_weights, biases),
        (),
        unit * (half_rows + medge_rows + 2 * senders_all),
    )

    given, held = call(
        functools.partial(land_kernel, exact, band_count, half_rows),
        [shape((half_rows + listed, width), BF16), shape((NEIGH, cap, width), BF16)],
        (enc_slot_node, other_lists, *landed),
        (),
        unit * (half_rows + listed),
    )
    kept, kept_listed = call(
        functools.partial(keep_kernel, band_count),
        [half_f, shape((listed, width), F32)],
        (enc_slot_node, lists, held),
        (),
        unit * (half_rows + listed),
    )
    got = swap(given, "band", 1)
    half = (kept + got[:half_rows].astype(F32)).astype(BF16)
    sums = (kept_listed + got[half_rows:].astype(F32)).astype(BF16)
    count = band_count // 2
    while True:
        count //= 2
        kept, given = sums[: count * senders_all], sums[count * senders_all :]
        got_listed = swap(given, "band", 2 * count)
        if count == 1:
            break
        sums = (kept.astype(F32) + got_listed.astype(F32)).astype(BF16)
    mask = 2
    while True:
        got = swap(half, "band", mask)
        if 2 * mask >= band_count:
            break
        half = crossed(half, got, share_rows, band_count, mask // 2)
        mask *= 2

    half_blocks = shape((blk_count // 2, mcap, width), BF16)
    kept, given = call(
        sender_kernel,
        [half_blocks, half_blocks],
        (
            kept,
            got_listed,
            listed_nodes,
            listed_part,
            enc_node_weights,
            proc_edge_weights,
            biases,
            gains,
        ),
        [pltpu.VMEM((blk_count, mcap, width), BF16)],
        unit * 3 * senders_all,
    )
    bit = 1
    while True:
        got_rows = swap(given, "blk", bit)
        senders = jnp.stack([kept, got_rows.reshape(kept.shape)], axis=1)
        bit *= 2
        if bit == blk_count:
            break
        view = senders.reshape(blk_count // (2 * bit), 2, bit * mcap, width)
        kept, given = view[:, 0], view[:, 1]
    arrived_senders = senders.reshape(senders_all, width)
    receivers = mesh_receiver.reshape(1, medge_rows)

    half_mid = call(
        functools.partial(node_kernel, band_count, mask // 2),
        half_bf,
        (half, got, nodes_by_share, node_part, enc_node_weights, biases, gains),
        (),
        unit * 2 * half_rows,
    )
    other_mid = swap(half_mid, "band", 1)

    mesh_part = call(
        functools.partial(target_kernel, band_count),
        shape((medge_rows, width), F32),
        (receivers, half_mid, other_mid, mesh_part, proc_edge_weights),
        [pltpu.VMEM((patch_rows, width), BF16)],
        unit * (patch_rows + medge_rows),
    )
    given, sent = call(
        functools.partial(process_kernel, band_count, mcap),
        [half_bf, shape((medge_rows, width), BF16)],
        (
            mesh_sender.reshape(1, medge_rows),
            receivers,
            mesh_part,
            arrived_senders,
            proc_edge_weights,
            biases,
            gains,
        ),
        (),
        unit * 2 * medge_rows,
    )
    kept, own_part = call(
        functools.partial(own_kernel, band_count),
        [half_f, shape((share_rows, width), F32)],
        (receivers, sent, half_mid, proc_node_weights, biases),
        (),
        unit * medge_rows,
    )
    got = swap(given, "band", 1)
    count = band_count // 2
    while count > 1:
        shares = kept + got.astype(F32)
        count //= 2
        kept, given = shares[: count * share_rows], shares[count * share_rows :].astype(BF16)
        got = swap(given, "band", 2 * count)
    mesh_out = call(
        last_kernel,
        shape((share_rows, width), BF16),
        (kept, got, half_mid, own_part, proc_node_weights, biases, gains),
        (),
        unit * 3 * share_rows,
    )
    return (grid_out, mesh_out)


def solution(mesh):
    rows = P(("blk", "band"), None)
    flat = P(("blk", "band"))
    in_specs = (rows, rows, flat, flat, rows, P("blk", None), rows, flat, flat, rows) + (P(),) * 7
    return jax.shard_map(body, mesh=mesh, in_specs=in_specs, out_specs=(rows, rows), check_vma=False)
```

```python
import functools

import jax
import jax.numpy as jnp
from jax import lax
from jax.experimental import pallas as pl
from jax.experimental.pallas import tpu as pltpu
from jax.sharding import PartitionSpec as P


NEIGH = 8
BF16 = jnp.bfloat16
F32 = jnp.float32
TILE = 512
GRANT = 16 << 20


def project(node_rows, weight):
    return jnp.dot(node_rows, weight, preferred_element_type=F32)


def silu(values):
    half = values * 0.5
    return half + half * jnp.tanh(half)


def normed(second, gain_row):
    center = second - jnp.mean(second, axis=-1, keepdims=True)
    spread = jnp.mean(center * center, axis=-1, keepdims=True)
    return center * (lax.rsqrt(spread + 1e-05) * gain_row)


def tail(first, weight, biases_ref, gains_ref, block):
    hidden = silu(first).astype(BF16)
    second = project(hidden, weight) + biases_ref[block, 1:2, :]
    return normed(second, gains_ref[block : block + 1, :])


def column(row):
    return jnp.broadcast_to(row, (128, row.shape[1])).T


def hot_columns(indices, names):
    wide = names.shape[1]
    if wide <= 128:
        return (indices[:, :wide] == names).astype(F32).astype(BF16)
    parts = [
        (indices == names[:, at : at + 128]).astype(F32).astype(BF16) for at in range(0, wide, 128)
    ]
    return jnp.concatenate(parts, axis=1)


def hot_rows(row, names):
    return (row == names).astype(F32).astype(BF16)


def lanes(count):
    return lax.broadcasted_iota(jnp.int32, (1, count), 1)


def sublanes(count):
    return lax.broadcasted_iota(jnp.int32, (count, 1), 0)


def share_names(iota, share_rows, band_count, core):
    half_count = band_count // 2
    x = lax.div(lax.axis_index("band"), 2)
    names = iota
    for place in range(band_count):
        share = 2 * ((place % half_count) ^ x) + (core if place < half_count else 1 - core)
        offset = (share - place) * share_rows
        inside = (iota >= place * share_rows) & (iota < (place + 1) * share_rows)
        names = jnp.where(inside, iota + offset, names)
    return names


def call(kernel, outs, args, scratch=(), flops=0, in_hbm=()):
    single = not isinstance(outs, (list, tuple))
    outs = [outs] if single else outs
    vmem = pl.BlockSpec(memory_space=pltpu.VMEM)
    args = [
        pltpu.with_memory_space_constraint(arg, pltpu.HBM if at in in_hbm else pltpu.VMEM)
        for at, arg in enumerate(args)
    ]
    results = pl.pallas_call(
        kernel,
        out_shape=tuple(pltpu.VMEM(out.shape, out.dtype) for out in outs),
        in_specs=[
            pl.BlockSpec(memory_space=pltpu.HBM) if at in in_hbm else vmem for at in range(len(args))
        ],
        out_specs=(vmem,) * len(outs),
        scratch_shapes=list(scratch),
        cost_estimate=pl.CostEstimate(flops=flops, transcendentals=0, bytes_accessed=0),
        compiler_params=pltpu.CompilerParams(vmem_limit_bytes=GRANT),
    )(*args)
    return results[0] if single else results


def shape(dims, kind):
    return jax.ShapeDtypeStruct(dims, kind)


def window_of(mask, exact):
    if not exact:
        return mask
    blk = lax.axis_index("blk")
    return lax.rem(blk - (blk ^ mask) + NEIGH // 2 + NEIGH, NEIGH)


def keys_kernel(exact, node_hbm, mesh_hbm, weights_hbm, *refs):
    outs, (held, nodes, mesh, weight, sems) = refs[:NEIGH], refs[NEIGH:]
    copies = [
        pltpu.make_async_copy(source, target, sems.at[at])
        for at, (source, target) in enumerate(
            ((node_hbm, nodes), (mesh_hbm, mesh), (weights_hbm.at[2], weight))
        )
    ]
    for copy in copies:
        copy.start()
    copies[0].wait()
    picks = hot_columns(column(nodes[...]), lanes(mesh.shape[0]))
    copies[1].wait()
    rows = project(picks, mesh[...]).astype(BF16)
    copies[2].wait()
    keys = project(rows, weight[...]).astype(BF16)
    held[...] = keys.reshape(held.shape)
    for mask in range(NEIGH):
        outs[mask][...] = held[window_of(mask, exact)]


def edge_kernel(sender_ref, grid_ref, weights_ref, biases_ref, edges_hbm, part_ref, edges, sems):
    tiles = range(0, edges.shape[0], TILE)
    copies = [
        pltpu.make_async_copy(
            edges_hbm.at[pl.ds(at, TILE), :], edges.at[pl.ds(at, TILE), :], sems.at[at // TILE]
        )
        for at in tiles
    ]
    for copy in copies:
        copy.start()
    names = lanes(grid_ref.shape[0])
    senders = column(sender_ref[...])
    for at, copy in zip(tiles, copies):
        picks = hot_columns(senders[at : at + TILE], names)
        nodes = project(picks, grid_ref[...]).astype(BF16)
        part = project(nodes, weights_ref[1]) + biases_ref[1, 0:1, :]
        copy.wait()
        part_ref[at : at + TILE, :] = part + project(edges[at : at + TILE, :], weights_ref[0])


def grid_kernel(grid_ref, weights_ref, biases_ref, gains_ref, out_ref):
    for at in range(0, grid_ref.shape[0], TILE):
        nodes = grid_ref[at : at + TILE, :]
        first = project(nodes, weights_ref[0]) + biases_ref[0, 0:1, :]
        out_ref[at : at + TILE, :] = (
            nodes.astype(F32) + tail(first, weights_ref[1], biases_ref, gains_ref, 0)
        ).astype(BF16)


def message_kernel(exact, slot_ref, part_ref, weights_ref, biases_ref, gains_ref, near_ref, far_ref, *refs):
    keys, outs, (lists_ref, table, sent) = refs[:NEIGH], refs[NEIGH : 2 * NEIGH], refs[2 * NEIGH :]
    lists_ref[: near_ref.shape[0], :] = near_ref[...]
    lists_ref[near_ref.shape[0] :, :] = far_ref[...]
    cap = keys[0].shape[0]
    for window in range(NEIGH):
        table[window * cap : (window + 1) * cap, :] = keys[window][...]
    row = slot_ref[...]
    if exact:
        blk = lax.axis_index("blk")
        patch = (lax.div(row, cap) + (blk + NEIGH // 2)) & (NEIGH - 1)
        row = (patch ^ blk) * cap + lax.rem(row, cap)
    slots = column(row)
    names = lanes(table.shape[0])
    for at in range(0, part_ref.shape[0], TILE):
        picks = hot_columns(slots[at : at + TILE], names)
        first = part_ref[at : at + TILE, :] + project(picks, table[...])
        sent[at : at + TILE, :] = tail(first, weights_ref[3], biases_ref, gains_ref, 1).astype(BF16)
    sums = project(hot_rows(row, sublanes(table.shape[0])), sent[...]).astype(BF16)
    for window in range(NEIGH):
        outs[window][...] = sums[window * cap : (window + 1) * cap, :]


def hot_lists(lists_ref, row):
    return jnp.concatenate(
        [
            hot_columns(column(lists_ref[at : at + 1, :]), row)
            for at in range(lists_ref.shape[0])
        ],
        axis=0,
    )


def listed_kernel(exact, node_ref, own_ref, other_ref, *refs):
    pieces, (given_ref, kept_ref, held) = refs[:NEIGH], refs[NEIGH:]
    for mask in range(NEIGH):
        held[window_of(mask, exact)] = pieces[mask][...]
    row = node_ref[...]
    landed = held[...].reshape(-1, held.shape[2])
    given_ref[...] = project(hot_lists(other_ref, row), landed).astype(BF16)
    kept_ref[...] = project(hot_lists(own_ref, row), landed)


def land_kernel(band_count, own, node_ref, held, sums_ref):
    half = sums_ref.shape[0]
    core = lax.rem(lax.axis_index("band"), 2)
    core = core if own else 1 - core
    names = share_names(sublanes(2 * half), 2 * half // band_count, band_count, core)
    landed = held[...].reshape(-1, held.shape[2])
    sums = project(hot_rows(node_ref[...], names[:half]), landed)
    sums_ref[...] = sums.astype(sums_ref.dtype)


def own_share(place):
    band = lax.axis_index("band")
    return 2 * (place ^ lax.div(band, 2)) + lax.rem(band, 2)


def early_kernel(
    band_count, send_ref, nodes_ref, edges_ref, w_nodes, w_edges, biases_ref, node_part_ref, edge_part_ref, listed_ref, listed_part_ref
):
    share = node_part_ref.shape[0] // (band_count // 2)
    nodes = nodes_ref[...].reshape(-1, nodes_ref.shape[2])
    rows = project(hot_columns(column(send_ref[...]), lanes(nodes.shape[0])), nodes).astype(BF16)
    listed_ref[...] = rows
    listed_part_ref[...] = project(rows, w_nodes[0]) + biases_ref[2, 0:1, :]
    for place in range(band_count // 2):
        node_part_ref[place * share : (place + 1) * share, :] = (
            project(nodes_ref[own_share(place)], w_nodes[0]) + biases_ref[2, 0:1, :]
        )
    for at in range(0, edges_ref.shape[0], TILE):
        edge_part_ref[at : at + TILE, :] = (
            project(edges_ref[at : at + TILE, :], w_edges[0]) + biases_ref[3, 0:1, :]
        )


def node_kernel(band_count, bit, half_ref, got_ref, nodes_ref, part_ref, weights_ref, biases_ref, gains_ref, out_ref):
    share = out_ref.shape[0] // (band_count // 2)
    total = crossed(half_ref, got_ref, share, band_count, bit)
    first = part_ref[...] + project(total, weights_ref[1])
    change = tail(first, weights_ref[2], biases_ref, gains_ref, 2)
    for place in range(band_count // 2):
        at = place * share
        out_ref[at : at + share, :] = (
            nodes_ref[own_share(place)].astype(F32) + change[at : at + share, :]
        ).astype(BF16)


def crossed(half, got, share, band_count, bit):
    parts = []
    for place in range(band_count // 2):
        at, other = place * share, (place ^ bit) * share
        parts.append(half[at : at + share, :].astype(F32) + got[other : other + share, :].astype(F32))
    return jnp.concatenate(parts, axis=0).astype(BF16)


def sender_kernel(
    sums_ref, got_ref, nodes_ref, part_ref, w_nodes, w_edges, biases_ref, gains_ref, kept_ref, given_ref, held
):
    total = (sums_ref[...].astype(F32) + got_ref[...].astype(F32)).astype(BF16)
    first = part_ref[...] + project(total, w_nodes[1])
    change = tail(first, w_nodes[2], biases_ref, gains_ref, 2)
    rows = (nodes_ref[...].astype(F32) + change).astype(BF16)
    held[...] = project(rows, w_edges[1]).astype(BF16).reshape(held.shape)
    blk = lax.axis_index("blk")
    for pair in range(kept_ref.shape[0]):
        kept_ref[pair] = held[blk ^ (2 * pair)]
        given_ref[pair] = held[blk ^ (2 * pair + 1)]


def target_kernel(band_count, receiver_ref, own_ref, other_ref, part_ref, weights_ref, out_ref, table):
    half = own_ref.shape[0]
    table[:half, :] = project(own_ref[...], weights_ref[2]).astype(BF16)
    table[half:, :] = project(other_ref[...], weights_ref[2]).astype(BF16)
    core = lax.rem(lax.axis_index("band"), 2)
    names = share_names(lanes(2 * half), 2 * half // band_count, band_count, core)
    receivers = column(receiver_ref[...])
    for at in range(0, part_ref.shape[0], TILE):
        picks = hot_columns(receivers[at : at + TILE], names)
        out_ref[at : at + TILE, :] = part_ref[at : at + TILE, :] + project(picks, table[...])


def process_kernel(
    band_count, mcap, sender_ref, receiver_ref, part_ref, keys_ref, weights_ref, biases_ref, gains_ref, given_ref, sent
):
    senders = column(sender_ref[...] ^ (lax.axis_index("blk") * mcap))
    names = lanes(keys_ref.shape[0])
    for at in range(0, part_ref.shape[0], TILE):
        picks = hot_columns(senders[at : at + TILE], names)
        first = part_ref[at : at + TILE, :] + project(picks, keys_ref[...])
        sent[at : at + TILE, :] = tail(first, weights_ref[3], biases_ref, gains_ref, 3).astype(BF16)
    given_ref[...] = half_sums(band_count, 0, 1, receiver_ref, sent, given_ref.shape[0]).astype(BF16)


def half_sums(band_count, own, far, receiver_ref, sent, count):
    core = lax.rem(lax.axis_index("band"), 2)
    core = core if own else 1 - core
    names = share_names(sublanes(4 * count), 4 * count // band_count, band_count, core)
    return project(hot_rows(receiver_ref[...], names[far * count : (far + 1) * count]), sent[...])


def far_kernel(band_count, receiver_ref, sent_ref, kept_ref):
    kept_ref[...] = half_sums(band_count, 1, 1, receiver_ref, sent_ref, kept_ref.shape[0])


def near_kernel(band_count, receiver_ref, sent_ref, half_ref, weights_ref, biases_ref, given_ref, kept_ref, part_ref):
    count = kept_ref.shape[0]
    given_ref[...] = half_sums(band_count, 0, 0, receiver_ref, sent_ref, count).astype(BF16)
    kept_ref[...] = half_sums(band_count, 1, 0, receiver_ref, sent_ref, count)
    part_ref[...] = project(half_ref[: part_ref.shape[0], :], weights_ref[0]) + biases_ref[4, 0:1, :]


def last_kernel(kept_ref, paired_ref, got_ref, half_ref, part_ref, weights_ref, biases_ref, gains_ref, out_ref):
    own = half_ref[: out_ref.shape[0], :]
    total = (kept_ref[...] + paired_ref[...].astype(F32) + got_ref[...].astype(F32)).astype(BF16)
    first = part_ref[...] + project(total, weights_ref[1])
    out_ref[...] = (
        own.astype(F32) + tail(first, weights_ref[2], biases_ref, gains_ref, 4)
    ).astype(BF16)


def swap(rows, axis, mask):
    return lax.ppermute(rows, axis, [(i, i ^ mask) for i in range(lax.axis_size(axis))])


def window_exchange(blocks, back):
    blk_count = lax.axis_size("blk")
    pieces = []
    for window in range(NEIGH):
        if blk_count == NEIGH:
            pieces.append(swap(blocks[window], "blk", window) if window else blocks[0])
        else:
            distance = window - NEIGH // 2
            distance = distance if back else -distance
            route = [((i - distance) % blk_count, i) for i in range(blk_count)]
            pieces.append(lax.ppermute(blocks[window], "blk", route) if distance else blocks[window])
    return pieces


def body(
    grid_nodes,
    enc_edges,
    enc_sender,
    enc_slot,
    enc_slot_node,
    mesh_nodes,
    mesh_edges,
    mesh_sender,
    mesh_receiver,
    mesh_send_node,
    grid_weights,
    enc_edge_weights,
    enc_node_weights,
    proc_edge_weights,
    proc_node_weights,
    biases,
    gains,
):
    blk_count, band_count = lax.axis_size("blk"), lax.axis_size("band")
    patch_rows, width = mesh_nodes.shape
    share_rows, half_rows = patch_rows // band_count, patch_rows // 2
    edge_rows, grid_rows, medge_rows = enc_edges.shape[0], grid_nodes.shape[0], mesh_edges.shape[0]
    slots = enc_slot_node.shape[1]
    cap = slots // NEIGH
    senders_all = mesh_send_node.shape[1]
    mcap = senders_all // blk_count
    for count in (blk_count, band_count, cap, mcap):
        assert count & (count - 1) == 0
    assert band_count >= 4
    exact = blk_count == NEIGH
    unit = 2 * width * width
    piece = shape((cap, width), BF16)
    half_bf, half_f = shape((half_rows, width), BF16), shape((half_rows, width), F32)

    slot_keys = call(
        functools.partial(keys_kernel, exact),
        [piece] * NEIGH,
        (enc_slot_node, mesh_nodes, enc_edge_weights),
        [
            pltpu.VMEM((NEIGH, cap, width), BF16),
            pltpu.VMEM((1, slots), jnp.int32),
            pltpu.VMEM((patch_rows, width), BF16),
            pltpu.VMEM((width, width), BF16),
            pltpu.SemaphoreType.DMA((3,)),
        ],
        unit * 2 * slots,
        (0, 1, 2),
    )
    keys = window_exchange(slot_keys, False)

    edge_part = call(
        edge_kernel,
        shape((edge_rows, width), F32),
        (enc_sender.reshape(1, edge_rows), grid_nodes, enc_edge_weights, biases, enc_edges),
        [pltpu.VMEM((edge_rows, width), BF16), pltpu.SemaphoreType.DMA((edge_rows // TILE,))],
        unit * 3 * edge_rows,
        (4,),
    )
    near, mask = mesh_send_node, 2
    while True:
        far = swap(near, "band", mask)
        mask *= 2
        if mask >= band_count:
            break
        near = jnp.concatenate([near, far], axis=0)
    *slot_sums, lists = call(
        functools.partial(message_kernel, exact),
        [piece] * NEIGH + [shape((band_count // 2, senders_all), jnp.int32)],
        (enc_slot.reshape(1, edge_rows), edge_part, enc_edge_weights, biases, gains, near, far, *keys),
        [pltpu.VMEM((slots, width), BF16), pltpu.VMEM((edge_rows, width), BF16)],
        unit * 3 * edge_rows,
    )
    landed = window_exchange(slot_sums, True)

    grid_out = call(
        grid_kernel,
        shape((grid_rows, width), BF16),
        (grid_nodes, grid_weights, biases, gains),
        (),
        unit * 2 * grid_rows,
    )
    other_lists = swap(lists, "band", 1)
    listed = band_count // 2 * senders_all

    nodes_by_share = mesh_nodes.reshape(band_count, share_rows, width)
    node_part, mesh_part, listed_nodes, listed_part = call(
        functools.partial(early_kernel, band_count),
        [half_f, shape((medge_rows, width), F32), shape((senders_all, width), BF16), shape((senders_all, width), F32)],
        (mesh_send_node, nodes_by_share, mesh_edges, enc_node_weights, proc_edge_weights, biases),
        (),
        unit * (half_rows + medge_rows + 2 * senders_all),
    )

    listed_shape = (listed, width)
    given, kept_listed, held = call(
        functools.partial(listed_kernel, exact),
        [shape(listed_shape, BF16), shape(listed_shape, F32), shape((NEIGH, cap, width), BF16)],
        (enc_slot_node, lists, other_lists, *landed),
        (),
        unit * 2 * listed,
    )
    got_listed = swap(given, "band", 1)
    given = call(functools.partial(land_kernel, band_count, 0), half_bf, (enc_slot_node, held), (), unit * half_rows)
    got = swap(given, "band", 1)
    kept = call(functools.partial(land_kernel, band_count, 1), half_f, (enc_slot_node, held), (), unit * half_rows)
    half = (kept + got.astype(F32)).astype(BF16)
    sums = (kept_listed + got_listed.astype(F32)).astype(BF16)
    count = band_count // 2
    while True:
        count //= 2
        kept, given = sums[: count * senders_all], sums[count * senders_all :]
        got_listed = swap(given, "band", 2 * count)
        if count == 1:
            break
        sums = (kept.astype(F32) + got_listed.astype(F32)).astype(BF16)
    mask = 2
    while True:
        got = swap(half, "band", mask)
        if 2 * mask >= band_count:
            break
        half = crossed(half, got, share_rows, band_count, mask // 2)
        mask *= 2

    half_blocks = shape((blk_count // 2, mcap, width), BF16)
    kept, given = call(
        sender_kernel,
        [half_blocks, half_blocks],
        (
            kept,
            got_listed,
            listed_nodes,
            listed_part,
            enc_node_weights,
            proc_edge_weights,
            biases,
            gains,
        ),
        [pltpu.VMEM((blk_count, mcap, width), BF16)],
        unit * 3 * senders_all,
    )
    bit = 1
    while True:
        got_rows = swap(given, "blk", bit)
        senders = jnp.stack([kept, got_rows.reshape(kept.shape)], axis=1)
        bit *= 2
        if bit == blk_count:
            break
        view = senders.reshape(blk_count // (2 * bit), 2, bit * mcap, width)
        kept, given = view[:, 0], view[:, 1]
    arrived_senders = senders.reshape(senders_all, width)
    receivers = mesh_receiver.reshape(1, medge_rows)

    half_mid = call(
        functools.partial(node_kernel, band_count, mask // 2),
        half_bf,
        (half, got, nodes_by_share, node_part, enc_node_weights, biases, gains),
        (),
        unit * 2 * half_rows,
    )
    other_mid = swap(half_mid, "band", 1)

    mesh_part = call(
        functools.partial(target_kernel, band_count),
        shape((medge_rows, width), F32),
        (receivers, half_mid, other_mid, mesh_part, proc_edge_weights),
        [pltpu.VMEM((patch_rows, width), BF16)],
        unit * (patch_rows + medge_rows),
    )
    count = band_count // 4
    near_rows = count * share_rows
    quarter_bf, quarter_f = shape((near_rows, width), BF16), shape((near_rows, width), F32)
    given, sent = call(
        functools.partial(process_kernel, band_count, mcap),
        [quarter_bf, shape((medge_rows, width), BF16)],
        (
            mesh_sender.reshape(1, medge_rows),
            receivers,
            mesh_part,
            arrived_senders,
            proc_edge_weights,
            biases,
            gains,
        ),
        (),
        unit * 2 * medge_rows,
    )
    got = swap(given, "band", 1)
    kept = call(functools.partial(far_kernel, band_count), quarter_f, (receivers, sent), (), unit * near_rows)
    given = (kept + got.astype(F32)).astype(BF16)
    got = swap(given, "band", 2 * count)
    given, kept, own_part = call(
        functools.partial(near_kernel, band_count),
        [quarter_bf, quarter_f, shape((share_rows, width), F32)],
        (receivers, sent, half_mid, proc_node_weights, biases),
        (),
        unit * medge_rows,
    )
    paired = swap(given, "band", 1)
    while count > 1:
        shares = kept + paired.astype(F32) + got.astype(F32)
        count //= 2
        kept, given = shares[: count * share_rows], shares[count * share_rows :].astype(BF16)
        paired = jnp.zeros_like(given)
        got = swap(given, "band", 2 * count)
    mesh_out = call(
        last_kernel,
        shape((share_rows, width), BF16),
        (kept, paired, got, half_mid, own_part, proc_node_weights, biases, gains),
        (),
        unit * 3 * share_rows,
    )
    return (grid_out, mesh_out)


def solution(mesh):
    rows = P(("blk", "band"), None)
    flat = P(("blk", "band"))
    in_specs = (rows, rows, flat, flat, rows, P("blk", None), rows, flat, flat, rows) + (P(),) * 7
    return jax.shard_map(body, mesh=mesh, in_specs=in_specs, out_specs=(rows, rows), check_vma=False)
```

```python
import functools

import jax
import jax.numpy as jnp
from jax import lax
from jax.experimental import pallas as pl
from jax.experimental.pallas import tpu as pltpu
from jax.sharding import PartitionSpec as P


NEIGH = 8
BF16 = jnp.bfloat16
F32 = jnp.float32
TILE = 512
GRANT = 16 << 20


def project(node_rows, weight):
    return jnp.dot(node_rows, weight, preferred_element_type=F32)


def silu(values):
    half = values * 0.5
    return half + half * jnp.tanh(half)


def normed(second, gain_row):
    center = second - jnp.mean(second, axis=-1, keepdims=True)
    spread = jnp.mean(center * center, axis=-1, keepdims=True)
    return center * (lax.rsqrt(spread + 1e-05) * gain_row)


def tail(first, weight, biases_ref, gains_ref, block):
    hidden = silu(first).astype(BF16)
    second = project(hidden, weight) + biases_ref[block, 1:2, :]
    return normed(second, gains_ref[block : block + 1, :])


def column(row):
    return jnp.broadcast_to(row, (128, row.shape[1])).T


def hot_columns(indices, names):
    wide = names.shape[1]
    if wide <= 128:
        return (indices[:, :wide] == names).astype(F32).astype(BF16)
    parts = [
        (indices == names[:, at : at + 128]).astype(F32).astype(BF16) for at in range(0, wide, 128)
    ]
    return jnp.concatenate(parts, axis=1)


def hot_rows(row, names):
    return (row == names).astype(F32).astype(BF16)


def lanes(count):
    return lax.broadcasted_iota(jnp.int32, (1, count), 1)


def sublanes(count):
    return lax.broadcasted_iota(jnp.int32, (count, 1), 0)


def share_names(iota, share_rows, band_count, core):
    half_count = band_count // 2
    x = lax.div(lax.axis_index("band"), 2)
    names = iota
    for place in range(band_count):
        share = 2 * ((place % half_count) ^ x) + (core if place < half_count else 1 - core)
        offset = (share - place) * share_rows
        inside = (iota >= place * share_rows) & (iota < (place + 1) * share_rows)
        names = jnp.where(inside, iota + offset, names)
    return names


def call(kernel, outs, args, scratch=(), flops=0, in_hbm=()):
    single = not isinstance(outs, (list, tuple))
    outs = [outs] if single else outs
    vmem = pl.BlockSpec(memory_space=pltpu.VMEM)
    args = [
        pltpu.with_memory_space_constraint(arg, pltpu.HBM if at in in_hbm else pltpu.VMEM)
        for at, arg in enumerate(args)
    ]
    results = pl.pallas_call(
        kernel,
        out_shape=tuple(pltpu.VMEM(out.shape, out.dtype) for out in outs),
        in_specs=[
            pl.BlockSpec(memory_space=pltpu.HBM) if at in in_hbm else vmem for at in range(len(args))
        ],
        out_specs=(vmem,) * len(outs),
        scratch_shapes=list(scratch),
        cost_estimate=pl.CostEstimate(flops=flops, transcendentals=0, bytes_accessed=0),
        compiler_params=pltpu.CompilerParams(vmem_limit_bytes=GRANT),
    )(*args)
    return results[0] if single else results


def shape(dims, kind):
    return jax.ShapeDtypeStruct(dims, kind)


def window_of(mask, exact):
    if not exact:
        return mask
    blk = lax.axis_index("blk")
    return lax.rem(blk - (blk ^ mask) + NEIGH // 2 + NEIGH, NEIGH)


def keys_kernel(exact, node_hbm, mesh_hbm, weights_hbm, *refs):
    outs, (held, nodes, mesh, weight, sems) = refs[:NEIGH], refs[NEIGH:]
    copies = [
        pltpu.make_async_copy(source, target, sems.at[at])
        for at, (source, target) in enumerate(
            ((node_hbm, nodes), (mesh_hbm, mesh), (weights_hbm.at[2], weight))
        )
    ]
    for copy in copies:
        copy.start()
    copies[0].wait()
    picks = hot_columns(column(nodes[...]), lanes(mesh.shape[0]))
    copies[1].wait()
    rows = project(picks, mesh[...]).astype(BF16)
    copies[2].wait()
    keys = project(rows, weight[...]).astype(BF16)
    held[...] = keys.reshape(held.shape)
    for mask in range(NEIGH):
        outs[mask][...] = held[window_of(mask, exact)]


def edge_kernel(sender_ref, grid_ref, weights_ref, biases_ref, edges_hbm, part_ref, edges, sems):
    tiles = range(0, edges.shape[0], TILE)
    copies = [
        pltpu.make_async_copy(
            edges_hbm.at[pl.ds(at, TILE), :], edges.at[pl.ds(at, TILE), :], sems.at[at // TILE]
        )
        for at in tiles
    ]
    for copy in copies:
        copy.start()
    names = lanes(grid_ref.shape[0])
    senders = column(sender_ref[...])
    for at, copy in zip(tiles, copies):
        picks = hot_columns(senders[at : at + TILE], names)
        nodes = project(picks, grid_ref[...]).astype(BF16)
        part = project(nodes, weights_ref[1]) + biases_ref[1, 0:1, :]
        copy.wait()
        part_ref[at : at + TILE, :] = part + project(edges[at : at + TILE, :], weights_ref[0])


def grid_kernel(grid_ref, weights_ref, biases_ref, gains_ref, out_ref):
    for at in range(0, grid_ref.shape[0], TILE):
        nodes = grid_ref[at : at + TILE, :]
        first = project(nodes, weights_ref[0]) + biases_ref[0, 0:1, :]
        out_ref[at : at + TILE, :] = (
            nodes.astype(F32) + tail(first, weights_ref[1], biases_ref, gains_ref, 0)
        ).astype(BF16)


def message_kernel(exact, slot_ref, part_ref, weights_ref, biases_ref, gains_ref, near_ref, far_ref, *refs):
    keys, outs, (lists_ref, table, sent) = refs[:NEIGH], refs[NEIGH : 2 * NEIGH], refs[2 * NEIGH :]
    lists_ref[: near_ref.shape[0], :] = near_ref[...]
    lists_ref[near_ref.shape[0] :, :] = far_ref[...]
    cap = keys[0].shape[0]
    for window in range(NEIGH):
        table[window * cap : (window + 1) * cap, :] = keys[window][...]
    row = slot_ref[...]
    if exact:
        blk = lax.axis_index("blk")
        patch = (lax.div(row, cap) + (blk + NEIGH // 2)) & (NEIGH - 1)
        row = (patch ^ blk) * cap + lax.rem(row, cap)
    slots = column(row)
    names = lanes(table.shape[0])
    for at in range(0, part_ref.shape[0], TILE):
        picks = hot_columns(slots[at : at + TILE], names)
        first = part_ref[at : at + TILE, :] + project(picks, table[...])
        sent[at : at + TILE, :] = tail(first, weights_ref[3], biases_ref, gains_ref, 1).astype(BF16)
    sums = project(hot_rows(row, sublanes(table.shape[0])), sent[...]).astype(BF16)
    for window in range(NEIGH):
        outs[window][...] = sums[window * cap : (window + 1) * cap, :]


def hot_lists(lists_ref, row):
    return jnp.concatenate(
        [
            hot_columns(column(lists_ref[at : at + 1, :]), row)
            for at in range(lists_ref.shape[0])
        ],
        axis=0,
    )


def listed_kernel(exact, node_ref, own_ref, other_ref, *refs):
    pieces, (given_ref, kept_ref, held) = refs[:NEIGH], refs[NEIGH:]
    for mask in range(NEIGH):
        held[window_of(mask, exact)] = pieces[mask][...]
    row = node_ref[...]
    landed = held[...].reshape(-1, held.shape[2])
    given_ref[...] = project(hot_lists(other_ref, row), landed).astype(BF16)
    kept_ref[...] = project(hot_lists(own_ref, row), landed)


def land_kernel(band_count, own, node_ref, held, sums_ref):
    half = sums_ref.shape[0]
    core = lax.rem(lax.axis_index("band"), 2)
    core = core if own else 1 - core
    names = share_names(sublanes(2 * half), 2 * half // band_count, band_count, core)
    landed = held[...].reshape(-1, held.shape[2])
    sums = project(hot_rows(node_ref[...], names[:half]), landed)
    sums_ref[...] = sums.astype(sums_ref.dtype)


def own_share(place):
    band = lax.axis_index("band")
    return 2 * (place ^ lax.div(band, 2)) + lax.rem(band, 2)


def early_kernel(
    band_count, send_ref, nodes_ref, edges_ref, w_nodes, w_edges, biases_ref, node_part_ref, edge_part_ref, listed_ref, listed_part_ref
):
    share = node_part_ref.shape[0] // (band_count // 2)
    nodes = nodes_ref[...].reshape(-1, nodes_ref.shape[2])
    rows = project(hot_columns(column(send_ref[...]), lanes(nodes.shape[0])), nodes).astype(BF16)
    listed_ref[...] = rows
    listed_part_ref[...] = project(rows, w_nodes[0]) + biases_ref[2, 0:1, :]
    for place in range(band_count // 2):
        node_part_ref[place * share : (place + 1) * share, :] = (
            project(nodes_ref[own_share(place)], w_nodes[0]) + biases_ref[2, 0:1, :]
        )
    for at in range(0, edges_ref.shape[0], TILE):
        edge_part_ref[at : at + TILE, :] = (
            project(edges_ref[at : at + TILE, :], w_edges[0]) + biases_ref[3, 0:1, :]
        )


def node_kernel(band_count, bit, half_ref, got_ref, nodes_ref, part_ref, weights_ref, biases_ref, gains_ref, out_ref):
    share = out_ref.shape[0] // (band_count // 2)
    total = crossed(half_ref, got_ref, share, band_count, bit)
    first = part_ref[...] + project(total, weights_ref[1])
    change = tail(first, weights_ref[2], biases_ref, gains_ref, 2)
    for place in range(band_count // 2):
        at = place * share
        out_ref[at : at + share, :] = (
            nodes_ref[own_share(place)].astype(F32) + change[at : at + share, :]
        ).astype(BF16)


def crossed(half, got, share, band_count, bit):
    parts = []
    for place in range(band_count // 2):
        at, other = place * share, (place ^ bit) * share
        parts.append(half[at : at + share, :].astype(F32) + got[other : other + share, :].astype(F32))
    return jnp.concatenate(parts, axis=0).astype(BF16)


def sender_kernel(
    sums_ref, got_ref, nodes_ref, part_ref, w_nodes, w_edges, biases_ref, gains_ref, kept_ref, given_ref, held
):
    total = (sums_ref[...].astype(F32) + got_ref[...].astype(F32)).astype(BF16)
    first = part_ref[...] + project(total, w_nodes[1])
    change = tail(first, w_nodes[2], biases_ref, gains_ref, 2)
    rows = (nodes_ref[...].astype(F32) + change).astype(BF16)
    held[...] = project(rows, w_edges[1]).astype(BF16).reshape(held.shape)
    blk = lax.axis_index("blk")
    count = kept_ref.shape[0]
    for place in range(count):
        kept_ref[place] = held[blk ^ place]
        given_ref[place] = held[blk ^ (count + place)]


def target_kernel(band_count, receiver_ref, own_ref, other_ref, part_ref, weights_ref, out_ref, table):
    half = own_ref.shape[0]
    table[:half, :] = project(own_ref[...], weights_ref[2]).astype(BF16)
    table[half:, :] = project(other_ref[...], weights_ref[2]).astype(BF16)
    core = lax.rem(lax.axis_index("band"), 2)
    names = share_names(lanes(2 * half), 2 * half // band_count, band_count, core)
    receivers = column(receiver_ref[...])
    for at in range(0, part_ref.shape[0], TILE):
        picks = hot_columns(receivers[at : at + TILE], names)
        out_ref[at : at + TILE, :] = part_ref[at : at + TILE, :] + project(picks, table[...])


def process_kernel(
    band_count, mcap, sender_ref, receiver_ref, part_ref, keys_ref, weights_ref, biases_ref, gains_ref, given_ref, sent
):
    senders = column(sender_ref[...] ^ (lax.axis_index("blk") * mcap))
    names = lanes(keys_ref.shape[0])
    for at in range(0, part_ref.shape[0], TILE):
        picks = hot_columns(senders[at : at + TILE], names)
        first = part_ref[at : at + TILE, :] + project(picks, keys_ref[...])
        sent[at : at + TILE, :] = tail(first, weights_ref[3], biases_ref, gains_ref, 3).astype(BF16)
    given_ref[...] = half_sums(band_count, 0, 1, receiver_ref, sent, given_ref.shape[0]).astype(BF16)


def half_sums(band_count, own, far, receiver_ref, sent, count):
    core = lax.rem(lax.axis_index("band"), 2)
    core = core if own else 1 - core
    names = share_names(sublanes(4 * count), 4 * count // band_count, band_count, core)
    return project(hot_rows(receiver_ref[...], names[far * count : (far + 1) * count]), sent[...])


def far_kernel(band_count, receiver_ref, sent_ref, kept_ref):
    kept_ref[...] = half_sums(band_count, 1, 1, receiver_ref, sent_ref, kept_ref.shape[0])


def near_kernel(band_count, receiver_ref, sent_ref, half_ref, weights_ref, biases_ref, given_ref, kept_ref, part_ref):
    count = kept_ref.shape[0]
    given_ref[...] = half_sums(band_count, 0, 0, receiver_ref, sent_ref, count).astype(BF16)
    kept_ref[...] = half_sums(band_count, 1, 0, receiver_ref, sent_ref, count)
    part_ref[...] = project(half_ref[: part_ref.shape[0], :], weights_ref[0]) + biases_ref[4, 0:1, :]


def last_kernel(kept_ref, paired_ref, got_ref, half_ref, part_ref, weights_ref, biases_ref, gains_ref, out_ref):
    own = half_ref[: out_ref.shape[0], :]
    total = (kept_ref[...] + paired_ref[...].astype(F32) + got_ref[...].astype(F32)).astype(BF16)
    first = part_ref[...] + project(total, weights_ref[1])
    out_ref[...] = (
        own.astype(F32) + tail(first, weights_ref[2], biases_ref, gains_ref, 4)
    ).astype(BF16)


def swap(rows, axis, mask):
    return lax.ppermute(rows, axis, [(i, i ^ mask) for i in range(lax.axis_size(axis))])


def window_exchange(blocks, back):
    blk_count = lax.axis_size("blk")
    pieces = []
    for window in range(NEIGH):
        if blk_count == NEIGH:
            pieces.append(swap(blocks[window], "blk", window) if window else blocks[0])
        else:
            distance = window - NEIGH // 2
            distance = distance if back else -distance
            route = [((i - distance) % blk_count, i) for i in range(blk_count)]
            pieces.append(lax.ppermute(blocks[window], "blk", route) if distance else blocks[window])
    return pieces


def body(
    grid_nodes,
    enc_edges,
    enc_sender,
    enc_slot,
    enc_slot_node,
    mesh_nodes,
    mesh_edges,
    mesh_sender,
    mesh_receiver,
    mesh_send_node,
    grid_weights,
    enc_edge_weights,
    enc_node_weights,
    proc_edge_weights,
    proc_node_weights,
    biases,
    gains,
):
    blk_count, band_count = lax.axis_size("blk"), lax.axis_size("band")
    patch_rows, width = mesh_nodes.shape
    share_rows, half_rows = patch_rows // band_count, patch_rows // 2
    edge_rows, grid_rows, medge_rows = enc_edges.shape[0], grid_nodes.shape[0], mesh_edges.shape[0]
    slots = enc_slot_node.shape[1]
    cap = slots // NEIGH
    senders_all = mesh_send_node.shape[1]
    mcap = senders_all // blk_count
    for count in (blk_count, band_count, cap, mcap):
        assert count & (count - 1) == 0
    assert band_count >= 4
    exact = blk_count == NEIGH
    unit = 2 * width * width
    piece = shape((cap, width), BF16)
    half_bf, half_f = shape((half_rows, width), BF16), shape((half_rows, width), F32)

    slot_keys = call(
        functools.partial(keys_kernel, exact),
        [piece] * NEIGH,
        (enc_slot_node, mesh_nodes, enc_edge_weights),
        [
            pltpu.VMEM((NEIGH, cap, width), BF16),
            pltpu.VMEM((1, slots), jnp.int32),
            pltpu.VMEM((patch_rows, width), BF16),
            pltpu.VMEM((width, width), BF16),
            pltpu.SemaphoreType.DMA((3,)),
        ],
        unit * 2 * slots,
        (0, 1, 2),
    )
    keys = window_exchange(slot_keys, False)

    edge_part = call(
        edge_kernel,
        shape((edge_rows, width), F32),
        (enc_sender.reshape(1, edge_rows), grid_nodes, enc_edge_weights, biases, enc_edges),
        [pltpu.VMEM((edge_rows, width), BF16), pltpu.SemaphoreType.DMA((edge_rows // TILE,))],
        unit * 3 * edge_rows,
        (4,),
    )
    near, mask = mesh_send_node, 2
    while True:
        far = swap(near, "band", mask)
        mask *= 2
        if mask >= band_count:
            break
        near = jnp.concatenate([near, far], axis=0)
    *slot_sums, lists = call(
        functools.partial(message_kernel, exact),
        [piece] * NEIGH + [shape((band_count // 2, senders_all), jnp.int32)],
        (enc_slot.reshape(1, edge_rows), edge_part, enc_edge_weights, biases, gains, near, far, *keys),
        [pltpu.VMEM((slots, width), BF16), pltpu.VMEM((edge_rows, width), BF16)],
        unit * 3 * edge_rows,
    )
    landed = window_exchange(slot_sums, True)

    grid_out = call(
        grid_kernel,
        shape((grid_rows, width), BF16),
        (grid_nodes, grid_weights, biases, gains),
        (),
        unit * 2 * grid_rows,
    )
    other_lists = swap(lists, "band", 1)
    listed = band_count // 2 * senders_all

    nodes_by_share = mesh_nodes.reshape(band_count, share_rows, width)
    node_part, mesh_part, listed_nodes, listed_part = call(
        functools.partial(early_kernel, band_count),
        [half_f, shape((medge_rows, width), F32), shape((senders_all, width), BF16), shape((senders_all, width), F32)],
        (mesh_send_node, nodes_by_share, mesh_edges, enc_node_weights, proc_edge_weights, biases),
        (),
        unit * (half_rows + medge_rows + 2 * senders_all),
    )

    listed_shape = (listed, width)
    given, kept_listed, held = call(
        functools.partial(listed_kernel, exact),
        [shape(listed_shape, BF16), shape(listed_shape, F32), shape((NEIGH, cap, width), BF16)],
        (enc_slot_node, lists, other_lists, *landed),
        (),
        unit * 2 * listed,
    )
    got_listed = swap(given, "band", 1)
    given = call(functools.partial(land_kernel, band_count, 0), half_bf, (enc_slot_node, held), (), unit * half_rows)
    got = swap(given, "band", 1)
    kept = call(functools.partial(land_kernel, band_count, 1), half_f, (enc_slot_node, held), (), unit * half_rows)
    half = (kept + got.astype(F32)).astype(BF16)
    sums = (kept_listed + got_listed.astype(F32)).astype(BF16)
    count = band_count // 2
    while True:
        count //= 2
        kept, given = sums[: count * senders_all], sums[count * senders_all :]
        got_listed = swap(given, "band", 2 * count)
        if count == 1:
            break
        sums = (kept.astype(F32) + got_listed.astype(F32)).astype(BF16)
    mask = 2
    while True:
        got = swap(half, "band", mask)
        if 2 * mask >= band_count:
            break
        half = crossed(half, got, share_rows, band_count, mask // 2)
        mask *= 2

    half_blocks = shape((blk_count // 2, mcap, width), BF16)
    kept, given = call(
        sender_kernel,
        [half_blocks, half_blocks],
        (
            kept,
            got_listed,
            listed_nodes,
            listed_part,
            enc_node_weights,
            proc_edge_weights,
            biases,
            gains,
        ),
        [pltpu.VMEM((blk_count, mcap, width), BF16)],
        unit * 3 * senders_all,
    )
    bit = blk_count // 2
    kept, given = kept.reshape(1, bit * mcap, width), given.reshape(1, bit * mcap, width)
    while True:
        got_rows = swap(given, "blk", bit)
        senders = jnp.stack([kept, got_rows], axis=1)
        bit //= 2
        if bit == 0:
            break
        view = senders.reshape(blk_count // (2 * bit), 2, bit * mcap, width)
        kept, given = view[:, 0], view[:, 1]
    arrived_senders = senders.reshape(senders_all, width)
    receivers = mesh_receiver.reshape(1, medge_rows)

    half_mid = call(
        functools.partial(node_kernel, band_count, mask // 2),
        half_bf,
        (half, got, nodes_by_share, node_part, enc_node_weights, biases, gains),
        (),
        unit * 2 * half_rows,
    )
    other_mid = swap(half_mid, "band", 1)

    mesh_part = call(
        functools.partial(target_kernel, band_count),
        shape((medge_rows, width), F32),
        (receivers, half_mid, other_mid, mesh_part, proc_edge_weights),
        [pltpu.VMEM((patch_rows, width), BF16)],
        unit * (patch_rows + medge_rows),
    )
    count = band_count // 4
    near_rows = count * share_rows
    quarter_bf, quarter_f = shape((near_rows, width), BF16), shape((near_rows, width), F32)
    given, sent = call(
        functools.partial(process_kernel, band_count, mcap),
        [quarter_bf, shape((medge_rows, width), BF16)],
        (
            mesh_sender.reshape(1, medge_rows),
            receivers,
            mesh_part,
            arrived_senders,
            proc_edge_weights,
            biases,
            gains,
        ),
        (),
        unit * 2 * medge_rows,
    )
    got = swap(given, "band", 1)
    kept = call(functools.partial(far_kernel, band_count), quarter_f, (receivers, sent), (), unit * near_rows)
    given = (kept + got.astype(F32)).astype(BF16)
    got = swap(given, "band", 2 * count)
    given, kept, own_part = call(
        functools.partial(near_kernel, band_count),
        [quarter_bf, quarter_f, shape((share_rows, width), F32)],
        (receivers, sent, half_mid, proc_node_weights, biases),
        (),
        unit * medge_rows,
    )
    paired = swap(given, "band", 1)
    while count > 1:
        shares = kept + paired.astype(F32) + got.astype(F32)
        count //= 2
        kept, given = shares[: count * share_rows], shares[count * share_rows :].astype(BF16)
        paired = jnp.zeros_like(given)
        got = swap(given, "band", 2 * count)
    mesh_out = call(
        last_kernel,
        shape((share_rows, width), BF16),
        (kept, paired, got, half_mid, own_part, proc_node_weights, biases, gains),
        (),
        unit * 3 * share_rows,
    )
    return (grid_out, mesh_out)


def solution(mesh):
    rows = P(("blk", "band"), None)
    flat = P(("blk", "band"))
    in_specs = (rows, rows, flat, flat, rows, P("blk", None), rows, flat, flat, rows) + (P(),) * 7
    return jax.shard_map(body, mesh=mesh, in_specs=in_specs, out_specs=(rows, rows), check_vma=False)
```
